256 devices in a mesh: row: 64 (over x, z, core), col: 4 (over y).
Axes of the slice: x: 4, y: 4, z: 8, core: 2. Of those that a mesh axis runs over, the one named last changes fastest.
Arguments:
- a_values: bfloat16 [16384, 16384], P('row', 'col'), may hold values from -0.046875 to 0.046875
- a_present: int32 [64, 64], P('row', 'col'), may hold values from 0 to 1, as said below
- b_values: bfloat16 [16384, 2048], P('row', 'col'), may hold values from -6 to 6
- b_present: int32 [64, 8], P('row', 'col'), may hold values 0 or 1
- w_values: bfloat16 [16384, 2048], P('row', 'col'), may hold values from -6 to 6
- w_present: int32 [64, 8], P('row', 'col'), may hold values 0 or 1
Outputs:
- masked: bfloat16 [16384, 2048], P('row', 'col')
- slot: float32 [64, 8], P('row', 'col')
- total: float32 [], replicated
The draws below stay inside these ranges and needn't reach their ends.
Inputs may be any that keep to these rules, and one draw needn't show every extreme that they name: `a_present`: 1 where a tile of a_values is present, else 0; the share of present tiles differs strongly from tile row to tile row.
All inputs are finite; a program needn't handle non-finite values. No bound on the sum of `b_present` or of `w_present` on one device may be relied on, other than what follows from the above.
Results may differ from the reference program's by a relative error of at most 0.001.
Values may be sent and summed in bfloat16 or wider, within the bound.
A program may use at most 128 MiB of HBM per device.

```python
import math
import jax
import jax.numpy as jnp

TILE = 256
TR_DEV = 1
TC_DEV = 2
MT = 64
KT = 64
NT = 8
N_ROW = 64
N_COL = 4


def draw_a_present(key, part):
    level_key = jax.random.fold_in(key, 11)
    roll_key = jax.random.fold_in(key, 23)
    level = jax.random.randint(level_key, (MT, 1), 1, 17)
    roll = jax.random.randint(roll_key, (MT, KT), 0, 16)
    return (roll < level).astype(jnp.int32)


def touch_ends(entries, rng, smallest, largest):
    longest = entries.shape.index(max(entries.shape))
    spots = []
    for shift in (0, 1):
        where = [jax.random.randint(jax.random.fold_in(rng, axis), (), 0, length) for axis, length in enumerate(entries.shape)]
        where[longest] = (where[longest] + shift) % entries.shape[longest]
        spots.append(tuple(where))
    return entries.at[spots[0]].set(smallest).at[spots[1]].set(largest)


def steps_of(stream_key, shape, split, least, largest):
    level, own = 1.0, jax.random.fold_in(stream_key, 6)
    for dim, parts in split:
        draws = jnp.exp(jax.random.uniform(jax.random.fold_in(own, dim), (parts,), jnp.float32, least / len(split), largest / len(split)))
        level = level * jnp.repeat(draws, shape[dim] // parts).reshape([-1 if axis == dim else 1 for axis in range(len(shape))])
    return level


def normal_values(stream_key, shape, width, most, pieces=(), kind=jnp.bfloat16):
    gain = steps_of(stream_key, shape, pieces, -0.22, 0.18) if pieces else 1.0
    drawn = jax.random.normal(stream_key, shape, jnp.float32) * width * gain
    return jnp.minimum(jnp.maximum(drawn, -most), most).astype(kind)


def setup_inputs(seed: int = 0) -> dict:
    key_list = jax.random.split(jax.random.key(seed), 7)
    return {
        "a_values": normal_values(key_list[0], (MT * TILE, KT * TILE), (KT * TILE) ** -0.5, 0.046875, ((0, 64), (1, 4))),
        "a_present": draw_a_present(jax.random.fold_in(key_list[6], 71), 0),
        "b_values": normal_values(key_list[2], (KT * TILE, NT * TILE), 1.0, 6.0, ((0, 64), (1, 4))),
        "b_present": touch_ends((jax.random.randint(key_list[3], (KT, NT), 0, 4) < 3).astype(jnp.int32), jax.random.fold_in(key_list[3], 1), 0, 1),
        "w_values": normal_values(key_list[4], (MT * TILE, NT * TILE), 1.0, 6.0, ((0, 64), (1, 4))),
        "w_present": touch_ends((jax.random.randint(key_list[5], (MT, NT), 0, 4) < 3).astype(jnp.int32), jax.random.fold_in(key_list[5], 1), 0, 1),
    }


def expand(values, present):
    tile_rows, tile_cols = present.shape
    tile_size = values.shape[0] // tile_rows
    blocked = values.reshape(tile_rows, tile_size, tile_cols, tile_size)
    masked_tiles = blocked * present.astype(values.dtype)[:, None, :, None]
    return masked_tiles.reshape(values.shape)

def reference(a_values, a_present, b_values, b_present, w_values, w_present):
    a_eff = expand(a_values, a_present)
    b_eff = expand(b_values, b_present)
    w_eff = expand(w_values, w_present)
    product = jnp.dot(a_eff, b_eff, preferred_element_type=jnp.float32)
    weighted = product * w_eff.astype(jnp.float32)
    masked = weighted.astype(jnp.bfloat16)
    tile_link = jnp.dot(a_present, b_present, preferred_element_type=jnp.int32)
    present = w_present * (tile_link > 0).astype(jnp.int32)
    ordered = present.reshape(N_ROW, TR_DEV, N_COL, TC_DEV).transpose(0, 2, 1, 3).reshape(-1)
    before = jnp.cumsum(ordered).astype(jnp.int32) - ordered
    slot_flat = jnp.where(ordered > 0, before, -1).astype(jnp.int32)
    slot = slot_flat.reshape(N_ROW, N_COL, TR_DEV, TC_DEV).transpose(0, 2, 1, 3).reshape(MT, NT)
    total = jnp.sum(weighted) / (TILE * math.sqrt(MT * NT))
    return (masked, slot.astype(jnp.float32), total)
```

```python
import functools
import heapq
import math

import jax
import jax.numpy as jnp
from jax import lax
from jax.experimental import pallas as pl
from jax.experimental.pallas import tpu as pltpu
from jax.sharding import PartitionSpec as P

MESH = pl.DeviceIdType.MESH
TILE = 256
NX, NZ, NY = 4, 8, 4
BLOCK = 1024
N1 = 384
ROWS = ((0, N1), (N1, BLOCK))
LINKS = ("x+", "x-", "z+", "z-")
LATENCY, RATE, LEAD = 2.2, 46.6e3, 3.0
RELAY = (0, -1, 2, -3)


def span(key):
    half, _, _, part = key
    first, last = ROWS[half]
    middle = (first + last) // 2
    return {"f": (first, last), "a": (first, middle), "b": (middle, last)}[part]


def plan():
    free = dict.fromkeys(LINKS, 0.0)
    waiting = {link: [] for link in LINKS}
    events, arrived, steps, count = [], {}, [], [0]

    def want(link, key, rank):
        count[0] += 1
        heapq.heappush(waiting[link], (rank, count[0], key))

    def send(now):
        out = []
        for link in LINKS:
            while waiting[link] and free[link] - now < LEAD:
                _, _, key = heapq.heappop(waiting[link])
                first, last = span(key)
                free[link] = max(now, free[link]) + (last - first) * 256 / RATE
                count[0] += 1
                heapq.heappush(events, (free[link] + LATENCY, count[0], key))
                out.append((link, key))
        return out

    def along_z(half, dx, dz):
        rank = abs(dx) if half == 0 else -1
        if dz == 0:
            want("z+", (half, dx, -1, "f"), rank)
            want("z-", (half, dx, 1, "f"), rank)
            return
        sign, link = (-1, "z+") if dz < 0 else (1, "z-")
        if abs(dz) < 3:
            want(link, (half, dx, dz + sign, "f"), rank)
        else:
            want(link, (half, dx, 4, "a" if sign < 0 else "b"), rank)

    along_z(1, 0, 0)
    want("x+", (0, -1, 0, "f"), -1)
    want("x-", (0, 1, 0, "f"), -1)
    along_z(0, 0, 0)
    want("x+", (1, -1, 0, "f"), 1)
    want("x-", (1, 1, 0, "f"), 1)
    steps.append((0.0, None, send(0.0)))
    while events:
        now, _, key = heapq.heappop(events)
        arrived[key] = now
        half, dx, dz, part = key
        whole = part == "f" or all((half, dx, dz, p) in arrived for p in "ab")
        if half == 0:
            if dz == 0:
                if dx == -1:
                    want("x+", (0, 2, 0, "a"), 0)
                if dx == 1:
                    want("x-", (0, 2, 0, "b"), 0)
                if whole:
                    along_z(0, dx, 0)
            elif part == "f":
                along_z(0, dx, dz)
        elif dx == 0:
            if part == "f":
                along_z(1, 0, dz)
            if whole:
                want("x+", (1, -1, dz, "f"), 1)
                want("x-", (1, 1, dz, "f"), 1)
        elif dx == -1 and dz in RELAY:
            want("x+", (1, 2, dz, "f"), 2)
        elif dx == 1 and dz not in RELAY:
            want("x-", (1, 2, dz, "f"), 2)
        steps.append((now, key, send(now)))
    return steps, arrived


STEPS, ARRIVED = plan()
KEYS = {key: n for n, key in enumerate(sorted(ARRIVED))}
BLOCKS = [(dx, dz) for dx in (0, -1, 1, 2) for dz in (0, -1, 1, -2, 2, -3, 3, 4)]
BLOCK_ID = {block: n for n, block in enumerate(BLOCKS)}
GROUP = {0: 0, -1: 1, 1: 2, 2: 3}


def program():
    items, need = [], {block: 0 for block in BLOCKS}
    for key in ARRIVED:
        need[key[1], key[2]] += 1
    complete = {}
    for now, key, sends in STEPS:
        items.append((now, 0, "step", (key, sends)))
        if key is not None:
            block = key[1], key[2]
            need[block] -= 1
            if need[block] == 0:
                complete[block] = now
                items.append((now, 1, "share", block))
    complete[0, 0] = 0.0
    items.append((0.0, 1, "share", (0, 0)))
    items.append((0.0, 2, "prepare", None))
    done = {}
    for block, now in sorted(complete.items(), key=lambda item: item[1]):
        items.append((now + 2.0, 3, "multiply", block))
        done.setdefault(block[0], []).append((now + 2.0, block))
    for dx, times in done.items():
        last = max(times)[0]
        items.append((last, 4, "scatter", dx))
        items.append((last + 10.0, 5, "store", dx))
    for stage in range(5):
        items.append((4.0 + 5.0 * stage, 6, "bits", stage))
    items.append((3.0, 6, "weights", None))
    final = max(times for times, *_ in items)
    items.append((max(max(times)[0] for times in done.values()), 4.5, "sum", None))
    items.sort(key=lambda item: (item[0], item[1]))
    return [(kind, what) for _, _, kind, what in items]


def kernel(
    a_ref, ap_ref, b_ref, bp_ref, w_ref, wp_ref,
    out_ref, slot_ref, total_ref,
    bg, ae, acc, rs, wa, bm, tot, iy, info, ta,
    a_sem, move_send, move_recv, piece_send, piece_recv, share_send, share_recv,
    w_send, w_recv, rs_send, rs_recv, info_send, info_recv, sum_send, sum_recv,
):
    row, y = lax.axis_index("row"), lax.axis_index("col")
    c = lax.rem(row, 2)
    z = lax.rem(row // 2, NZ)
    x = row // (2 * NZ)

    def device(dx=0, dy=0, dz=0, dc=0):
        xx, zz = lax.rem(x + dx + NX, NX), lax.rem(z + dz + NZ, NZ)
        return ((xx * NZ + zz) * 2 + lax.rem(c + dc, 2), lax.rem(y + dy + NY, NY))

    def place(xx, yy):
        return ((xx * NZ + z) * 2 + c, yy)

    def remote(src, dst, send, recv, to):
        return pltpu.make_async_remote_copy(
            src_ref=src, dst_ref=dst, send_sem=send, recv_sem=recv,
            device_id=to, device_id_type=MESH,
        )

    sent = []

    def go(*args):
        copy = remote(*args)
        copy.start()
        sent.append(copy)

    barrier = pltpu.get_barrier_semaphore()

    def greet(to):
        pl.semaphore_signal(barrier, inc=1, device_id=to, device_id_type=MESH)

    loads = []
    for k in range(NZ):
        load = pltpu.make_async_copy(
            a_ref.at[:, pl.ds(k * 2 * TILE, 2 * TILE)], ae.at[k], a_sem.at[k]
        )
        load.start()
        loads.append(load)
    for d in range(1, NY):
        greet(device(dy=d))
    for d in range(1, NX):
        greet(device(dx=d))
    for d in range(1, NZ):
        greet(device(dz=d))
    greet(device(dc=1))
    diagonal = x == y
    for q in range(NX):
        own = diagonal & (x == q)

        @pl.when(jnp.logical_not(own))
        def _():
            greet(place(q, x))
            greet(place(y, q))

    def flag(ref, n):
        return ref[0, n].astype(jnp.float32).astype(jnp.bfloat16)

    for t in range(2):
        cols = pl.ds(t * TILE, TILE)
        bm[:, cols] = b_ref[:, cols] * flag(bp_ref, t)
    for q in range(NX):
        wa[y, q] = w_ref[:, pl.ds(q * 128, 128)] * flag(wp_ref, q // 2)
    lane = lax.broadcasted_iota(jnp.int32, (1, 128), 1)
    bits = jnp.zeros((1, 128), jnp.float32)
    for t in range(16):
        bits = jnp.where(lane == 16 * y + t, ap_ref[0, t].astype(jnp.float32), bits)
    for t in range(2):
        both = wp_ref[0, t] + 2 * bp_ref[0, t]
        bits = jnp.where(lane == 64 + 2 * y + t, both.astype(jnp.float32), bits)
    iy[0] = bits
    pl.semaphore_wait(barrier, 14 + jnp.where(diagonal, 6, 8))

    for q in range(NX):
        own = diagonal & (x == q)
        rows = pl.ds(pl.multiple_of(y * TILE, TILE), TILE)

        @pl.when(jnp.logical_not(own))
        def _():
            remote(
                bm.at[:, pl.ds(q * 128, 128)], bg.at[q, z, c, rows],
                move_send.at[q], move_recv.at[y], place(q, x),
            ).start()

        @pl.when(own)
        def _():
            bg[q, z, c, rows] = bm[:, pl.ds(q * 128, 128)]

    for q in range(NY):
        own = diagonal & (y == q)

        @pl.when(jnp.logical_not(own))
        def _():
            dst = bg.at[x, z, c, pl.ds(q * TILE, TILE)]
            remote(dst, dst, move_send.at[0], move_recv.at[q], place(y, q)).wait_recv()

    def block(dx, dz):
        return lax.rem(x + dx + NX, NX), lax.rem(z + dz + NZ, NZ)

    def piece(key, dx=0, dz=0):
        first, last = span(key)
        xx, zz = block(key[1] + dx, key[2] + dz)
        return bg.at[xx, zz, c, pl.ds(first, last - first)]

    def step(what):
        key, sends = what
        if key is not None:
            n, dst = KEYS[key], piece(key)
            remote(dst, dst, piece_send.at[n], piece_recv.at[n], device(dc=1)).wait_recv()
        for link, out in sends:
            d = 1 if link[1] == "+" else -1
            to = {"dx": d} if link[0] == "x" else {"dz": d}
            ref, n = piece(out, **to), KEYS[out]
            go(ref, ref, piece_send.at[n], piece_recv.at[n], device(**to))

    def share(what):
        n, (xx, zz) = BLOCK_ID[what], block(*what)
        ref = bg.at[xx, zz, c]
        go(ref, ref, share_send.at[n], share_recv.at[n], device(dc=1))

    def prepare(_):
        for k in range(NZ):
            loads[k].wait()
            for t in range(2):
                cols = pl.ds(t * TILE, TILE)
                ae[k, :, cols] = ae[k, :, cols] * flag(ap_ref, 2 * k + t)

    begun = set()

    def multiply(what):
        n, (xx, zz) = BLOCK_ID[what], block(*what)
        ref = bg.at[xx, zz, 1 - c]
        remote(ref, ref, share_send.at[n], share_recv.at[n], device(dc=1)).wait_recv()
        group = GROUP[what[0]]
        fresh = group not in begun
        begun.add(group)

        def pair(p, carry):
            def part(core, t):
                start = pl.multiple_of((2 * p + t) * TILE, TILE)
                return bg[xx, zz, core, pl.ds(start, TILE), :]

            right = jnp.concatenate(
                [jnp.concatenate([part(k, 0), part(k, 1)], axis=1) for k in range(2)], axis=0
            )
            new = jnp.dot(ae[zz], right, preferred_element_type=jnp.float32)
            for t in range(2):
                new_t = new[:, t * 128 : (t + 1) * 128]
                acc[group, 2 * p + t] = new_t if fresh else acc[group, 2 * p + t] + new_t
            return carry

        lax.fori_loop(0, 2, pair, 0)

    def weights(_):
        for d in range(1, NY):
            go(wa.at[y], wa.at[y], w_send.at[d - 1], w_recv.at[d - 1], device(dy=d))

    heard = []

    def scatter(dx):
        group, xx = GROUP[dx], block(dx, 0)[0]
        for d in range(1, NY):
            yb = lax.rem(y + d, NY)
            n = (d - 1) * NX + group
            go(
                acc.at[group, yb], rs.at[d - 1, group],
                rs_send.at[n], rs_recv.at[n], device(dy=d),
            )
        if not heard:
            heard.append(True)
            tot[...] = jnp.zeros_like(tot)
            for d in range(1, NY):
                ref = wa.at[lax.rem(y + NY - d, NY)]
                remote(ref, ref, w_send.at[d - 1], w_recv.at[d - 1], device(dy=d)).wait_recv()

        def one(yb, carry):
            value = acc[group, yb] * wa[yb, xx].astype(jnp.float32)
            tot[...] += jnp.sum(value.reshape(TILE // 8, 8, 128), axis=0)
            return carry

        lax.fori_loop(0, NY, one, 0)

    def store(dx):
        group, xx = GROUP[dx], block(dx, 0)[0]
        value = acc[group, y]
        for d in range(1, NY):
            n = (d - 1) * NX + group
            ref = rs.at[d - 1, group]
            remote(ref, ref, rs_send.at[n], rs_recv.at[n], device(dy=d)).wait_recv()
            value = value + rs[d - 1, group]
        value = value * wa[y, xx].astype(jnp.float32)
        out_ref[:, pl.ds(pl.multiple_of(xx * 128, 128), 128)] = value.astype(jnp.bfloat16)

    def peers(stage):
        return {
            "y": [(d - 1, {"dy": d}) for d in range(1, NY)],
            "c": [(3, {"dc": 1})],
            "x": [(3 + d, {"dx": d}) for d in range(1, NX)],
            "z": [(6 + d, {"dz": d}) for d in range(1, NZ)],
        }[stage]

    def info_refs(stage, to, back):
        s = -1 if back else 0
        if stage == "y":
            n = to["dy"]
            return (iy.at[0], iy.at[n])
        if stage == "c":
            ref = info.at[z, x, lax.rem(c + 1, 2) if back else c]
        elif stage == "x":
            ref = info.at[z, lax.rem(x + s * to["dx"] + NX, NX)]
        else:
            ref = info.at[lax.rem(z + s * to["dz"] + NZ, NZ)]
        return ref, ref

    def bits_stage(stage):
        order = "ycxz"
        if stage > 0:
            for n, to in peers(order[stage - 1]):
                ref = info_refs(order[stage - 1], to, True)[1]
                remote(ref, ref, info_send.at[n], info_recv.at[n], device(dc=1)).wait_recv()
        if stage == 1:
            info[z, x, c] = iy[0] + iy[1] + iy[2] + iy[3]
        if stage < 4:
            for n, to in peers(order[stage]):
                src, dst = info_refs(order[stage], to, False)
                go(src, dst, info_send.at[n], info_recv.at[n], device(**to))
            return
        at = lax.broadcasted_iota(jnp.int32, (64, 128), 0)
        lanes = lax.broadcasted_iota(jnp.int32, (64, 128), 1)
        table = jnp.zeros((64, 128), jnp.float32)
        for i in range(64):
            xi, zi, ci = i // 16, (i // 2) % 8, i % 2
            table = jnp.where(at == i, info[zi, xi, ci], table)
        tail = lanes >= 64
        bp = jnp.where(tail & (table > 1.5), 1.0, 0.0)
        wp = jnp.where(tail, table - 2.0 * bp, 0.0)
        ap = jnp.where(tail, 0.0, table).astype(jnp.bfloat16)
        wide = jnp.concatenate([bp, jnp.zeros_like(bp)], axis=0).astype(jnp.bfloat16)
        link = jnp.dot(ap, wide, preferred_element_type=jnp.float32)
        present = jnp.where(link > 0.5, wp, 0.0)
        left = (
            lax.broadcasted_iota(jnp.int32, (128, 128), 0)
            < lax.broadcasted_iota(jnp.int32, (128, 128), 1)
        )
        marks = present.astype(jnp.bfloat16)
        inside = jnp.dot(marks, jnp.where(left, 1.0, 0.0).astype(jnp.bfloat16),
                         preferred_element_type=jnp.float32)
        mine = at == row
        earlier = jnp.sum(jnp.where(at < row, present, 0.0))
        before = jnp.sum(jnp.where(mine, inside, 0.0), axis=0, keepdims=True) + earlier
        here = jnp.sum(jnp.where(mine, present, 0.0), axis=0, keepdims=True)
        slots = jnp.where(here > 0.5, before, -1.0)
        pick = lambda t: jnp.sum(jnp.where(lane == 64 + 2 * y + t, slots, 0.0), axis=1, keepdims=True)
        slot_ref[...] = jnp.concatenate([pick(0), pick(1)], axis=1)

    def sum_stages(_):
        value = jnp.sum(tot[...], axis=0, keepdims=True)
        at = {"c": (0, 2, c), "y": (2, NY, y), "x": (6, NX, x), "z": (10, NZ, z)}
        for stage in "cyxz":
            base, size, me = at[stage]
            ta[base + me] = value
            for n, to in peers(stage):
                ref = ta.at[base + me]
                go(ref, ref, sum_send.at[n], sum_recv.at[n], device(**to))
            for n, to in peers(stage):
                back = lax.rem(me + size - next(iter(to.values())), size)
                ref = ta.at[base + back]
                remote(ref, ref, sum_send.at[n], sum_recv.at[n], device(dc=1)).wait_recv()
            value = ta[base]
            for k in range(1, size):
                value = value + ta[base + k]
        total_ref[0, 0] = jnp.sum(value) / (TILE * math.sqrt(64 * 8))

    run = {
        "step": step, "share": share, "prepare": prepare, "multiply": multiply,
        "weights": weights, "scatter": scatter, "store": store, "bits": bits_stage,
        "sum": sum_stages,
    }
    for kind, what in program():
        run[kind](what)
    for copy in sent:
        copy.wait_send()
    for q in range(NX):
        own = diagonal & (x == q)

        @pl.when(jnp.logical_not(own))
        def _():
            src = bm.at[:, pl.ds(q * 128, 128)]
            remote(src, src, move_send.at[q], move_recv.at[0], place(q, x)).wait_send()


def on_device(a_values, a_present, b_values, b_present, w_values, w_present):
    vmem = pl.BlockSpec(memory_space=pltpu.VMEM)
    smem = pl.BlockSpec(memory_space=pltpu.SMEM)
    dma = pltpu.SemaphoreType.DMA
    masked, slot, total = pl.pallas_call(
        kernel,
        out_shape=(
            jax.ShapeDtypeStruct((TILE, 512), jnp.bfloat16),
            jax.ShapeDtypeStruct((1, 2), jnp.float32),
            jax.ShapeDtypeStruct((1, 1), jnp.float32),
        ),
        in_specs=[pl.BlockSpec(memory_space=pl.ANY), smem, vmem, smem, vmem, smem],
        out_specs=(vmem, vmem, smem),
        scratch_shapes=[
            pltpu.VMEM((NX, NZ, 2, BLOCK, 128), jnp.bfloat16),
            pltpu.VMEM((NZ, TILE, 2 * TILE), jnp.bfloat16),
            pltpu.VMEM((NX, NY, TILE, 128), jnp.float32),
            pltpu.VMEM((NY - 1, NX, TILE, 128), jnp.float32),
            pltpu.VMEM((NY, NX, TILE, 128), jnp.bfloat16),
            pltpu.VMEM((TILE, 512), jnp.bfloat16),
            pltpu.VMEM((8, 128), jnp.float32),
            pltpu.VMEM((NY, 1, 128), jnp.float32),
            pltpu.VMEM((NZ, NX, 2, 1, 128), jnp.float32),
            pltpu.VMEM((18, 1, 128), jnp.float32),
            dma((NZ,)), dma((NX,)), dma((NY,)),
            dma((len(KEYS),)), dma((len(KEYS),)),
            dma((len(BLOCKS),)), dma((len(BLOCKS),)),
            dma((3,)), dma((3,)), dma((12,)), dma((12,)),
            dma((14,)), dma((14,)), dma((14,)), dma((14,)),
        ],
        compiler_params=pltpu.CompilerParams(
            collective_id=0, has_side_effects=True, vmem_limit_bytes=50 * 2**20
        ),
    )(a_values, a_present, b_values, b_present, w_values, w_present)
    return masked, slot, total.reshape(())


def solution(mesh):
    spec = P("row", "col")
    return jax.shard_map(
        on_device, mesh=mesh, in_specs=(spec,) * 6, out_specs=(spec, spec, P()),
        check_vma=False,
    )
```

```python
import heapq
import math

import jax
import jax.numpy as jnp
from jax import lax
from jax.experimental import pallas as pl
from jax.experimental.pallas import tpu as pltpu
from jax.sharding import PartitionSpec as P

MESH = pl.DeviceIdType.MESH
TILE = 256
NX, NZ, NY = 4, 8, 4
LINKS = ("x+", "x-", "z+", "z-")
PIECES = (
    (True, 0, 256, 0),
    (True, 256, 256, 1),
    (True, 768, 128, 3),
    (False, 512, 256, 2),
    (False, 896, 128, 3),
)
BLOCKS = [(dx, dz) for dx in (0, -1, 1, 2) for dz in (0, -1, 1, -2, 2, -3, 3, 4)]
BLOCK_ID = {block: n for n, block in enumerate(BLOCKS)}
GROUP = {0: 0, -1: 1, 1: 2, 2: 3}
KEY_ID = {
    key: n for n, key in enumerate((p, *block) for p in range(len(PIECES)) for block in BLOCKS)
}
LATENCY, RATE, LEAD = 2.8, 46.6e3, 3.0
STEP, ISSUE, MULTIPLY, SHARE = 0.03, 0.02, 0.47, 1.5
READY = (0.0, 0.6, 1.2, 1.8, 1.2)
X_FIRST_RANK = (0, 1, 2)
X_RANK = (1, 2)
BITS = (1.0, 9.0, 17.0, 26.0, 40.0)
SUMS = (0.0, 1.2, 3.8, 5.0, 3.8)


def program():
    free = dict.fromkeys(LINKS + ("y+", "y-"), 0.0)
    waiting = {link: [] for link in LINKS}
    inbox, ready, items, count = [], [], [], [0]
    missing = {block: len(PIECES) for block in BLOCKS}
    left = {dx: NZ for dx in GROUP}

    def push(heap, when, what):
        count[0] += 1
        heapq.heappush(heap, (when, count[0], what))

    def commit(now):
        sends = []
        for link in LINKS:
            while waiting[link] and free[link] - now < LEAD:
                key = heapq.heappop(waiting[link])[2]
                free[link] = max(now, free[link]) + PIECES[key[0]][2] * 256 / RATE
                push(inbox, free[link] + LATENCY, key)
                sends.append((link, key))
        return tuple(sends)

    def along_y(link, now, rows):
        free[link] = max(now, free[link]) + rows * 512 / RATE
        return free[link] + LATENCY

    def along_z(p, dx, dz):
        rank = -1 if PIECES[p][0] else X_FIRST_RANK[abs(dx)]
        if dz == 0:
            push(waiting["z+"], rank, (p, dx, -1))
            push(waiting["z-"], rank, (p, dx, 1))
        elif abs(dz) < 3:
            sign = 1 if dz > 0 else -1
            push(waiting["z-" if dz > 0 else "z+"], rank, (p, dx, dz + sign))
        elif abs(dz) == 3:
            sign = -1 if (p + abs(dx) // 2 + (dx == 1)) % 2 == 0 else 1
            if (dz < 0) == (sign < 0):
                push(waiting["z-" if dz > 0 else "z+"], rank, (p, dx, 4))

    def along_x(p, dx, dz):
        if dx == 0:
            rank = X_RANK[0] if PIECES[p][0] else -1
            push(waiting["x+"], rank, (p, -1, dz))
            push(waiting["x-"], rank, (p, 1, dz))
        elif dx == (-1 if (p + dz) % 2 == 0 else 1):
            rank = X_RANK[1] if PIECES[p][0] else 0
            push(waiting["x+" if dx < 0 else "x-"], rank, (p, 2, dz))

    for p, when in enumerate(READY):
        push(inbox, when, (p, 0, 0))
    for stage, when in enumerate(BITS):
        push(ready, when, ("bits", stage))
    push(ready, 3.0, ("weights", None))
    push(ready, 2.5, ("prepare", None))
    now, stage = 0.0, 0
    while inbox or ready:
        if inbox and inbox[0][0] <= now:
            key = heapq.heappop(inbox)[2]
            p, dx, dz = key
            if PIECES[p][0]:
                if dx == 0:
                    along_z(*key)
                along_x(*key)
            else:
                if dz == 0:
                    along_x(*key)
                along_z(*key)
            now += STEP
            sends = commit(now)
            now += ISSUE * len(sends)
            items.append(("step", (key, sends)))
            block = dx, dz
            missing[block] -= 1
            if missing[block] == 0:
                items.append(("share", block))
                push(ready, now + SHARE, ("multiply", block))
        elif ready and ready[0][0] <= now:
            kind, what = heapq.heappop(ready)[2]
            items.append((kind, what))
            if kind == "multiply":
                now += MULTIPLY
                dx = what[0]
                left[dx] -= 1
                if left[dx] == 0:
                    items.append(("scatter", dx))
                    now += 0.25
                    first = max(along_y("y+", now, 128), along_y("y-", now, 128))
                    along_y("y+", now, 128), along_y("y-", now, 128)
                    push(ready, first, ("add", dx))
                    if not any(left.values()):
                        push(ready, now, ("sum", 0))
            elif kind == "add":
                now += 0.15
                last = max(along_y("y+", now, 128), along_y("y-", now, 128))
                push(ready, last, ("store", what))
            elif kind == "sum" and what < 4:
                push(ready, now + SUMS[what + 1], ("sum", what + 1))
            elif kind == "prepare":
                now += 0.3
            elif kind == "store":
                now += 0.1
            sends = commit(now)
            if sends:
                items.append(("step", (None, sends)))
        else:
            now = min(heap[0][0] for heap in (inbox, ready) if heap)
    program.end = now
    return items


def kernel(
    a_ref, ap_ref, b_ref, bp_ref, w_ref, wp_ref,
    out_ref, slot_ref, total_ref,
    bg, ae, acc, rl, rs, wa, bm, braw, wraw, masked, tot, iy, info, ta, ap, bp, wp,
    a_sem, in_sem, out_sem, move_send, move_recv, piece_send, piece_recv, share_send, share_recv,
    w_send, w_recv, rs_send, rs_recv, info_send, info_recv, sum_send, sum_recv,
):
    row, y = lax.axis_index("row"), lax.axis_index("col")
    c = lax.rem(row, 2)
    z = lax.rem(row // 2, NZ)
    x = row // (2 * NZ)

    def device(dx=0, dy=0, dz=0, dc=0):
        xx, zz = lax.rem(x + dx + NX, NX), lax.rem(z + dz + NZ, NZ)
        return ((xx * NZ + zz) * 2 + lax.rem(c + dc, 2), lax.rem(y + dy + NY, NY))

    def place(xx, yy):
        return ((xx * NZ + z) * 2 + c, yy)

    def remote(src, dst, send, recv, to):
        return pltpu.make_async_remote_copy(
            src_ref=src, dst_ref=dst, send_sem=send, recv_sem=recv,
            device_id=to, device_id_type=MESH,
        )

    def arrive(dst, recv):
        remote(dst, dst, sum_send.at[0], recv, device(dc=1)).wait_recv()

    sent = []

    def go(*args):
        copy = remote(*args)
        copy.start()
        sent.append(copy)

    loads = [
        pltpu.make_async_copy(src, dst, in_sem.at[n])
        for n, (src, dst) in enumerate(
            ((b_ref, braw), (bp_ref, bp), (ap_ref, ap), (wp_ref, wp), (w_ref, wraw))
        )
    ]
    for k in range(NZ):
        loads.append(pltpu.make_async_copy(
            a_ref.at[:, pl.ds(k * 2 * TILE, 2 * TILE)], ae.at[k], a_sem.at[k]
        ))
    for load in loads:
        load.start()
    barrier = pltpu.get_barrier_semaphore()

    def greet(to):
        pl.semaphore_signal(barrier, inc=1, device_id=to, device_id_type=MESH)

    diagonal = x == y
    for d in range(1, NZ):
        greet(device(dz=d))
    for d in range(1, NX):
        greet(device(dx=d))
    for d in range(1, NY):
        greet(device(dy=d))
    greet(device(dc=1))
    for q in range(NX):

        @pl.when(jnp.logical_not(diagonal & (x == q)))
        def _():
            greet(place(q, x))
            greet(place(y, q))

    def flag(ref, n):
        return ref[0, n].astype(jnp.float32).astype(jnp.bfloat16)

    for load in loads[:2]:
        load.wait()
    for q in range(NX):
        bm[q] = braw[:, pl.ds(q * 128, 128)] * flag(bp, q // 2)
    for load in loads[2:4]:
        load.wait()
    lane = lax.broadcasted_iota(jnp.int32, (1, 128), 1)
    bits = jnp.zeros((1, 128), jnp.float32)
    for t in range(16):
        bits = jnp.where(lane == 16 * y + t, ap[0, t].astype(jnp.float32), bits)
    for t in range(2):
        both = wp[0, t] + 2 * bp[0, t]
        bits = jnp.where(lane == 64 + 2 * y + t, both.astype(jnp.float32), bits)
    iy[0] = bits
    pl.semaphore_wait(barrier, 14 + jnp.where(diagonal, 6, 8))

    mine = lax.rem(y - x + NY, NY)
    rows = pl.ds(pl.multiple_of(mine * TILE, TILE), TILE)

    def move(d):
        q = lax.rem(x + d, NX)
        return remote(
            bm.at[q], bg.at[q, z, c, rows], move_send.at[d], move_recv.at[mine], place(q, x)
        )

    for d in (2, 1, 3):
        move(d).start()

    @pl.when(jnp.logical_not(diagonal))
    def _():
        move(0).start()

    @pl.when(diagonal)
    def _():
        bg[x, z, c, rows] = bm[x]

    landed = set()

    def land(j):
        if j in landed:
            return
        landed.add(j)
        dst = bg.at[x, z, c, pl.ds(j * TILE, TILE)]
        if j > 0:
            arrive(dst, move_recv.at[j])
            return

        @pl.when(jnp.logical_not(diagonal))
        def _():
            arrive(dst, move_recv.at[0])

    def block(dx, dz):
        return lax.rem(x + dx + NX, NX), lax.rem(z + dz + NZ, NZ)

    def piece(key, dx=0, dz=0):
        _, first, size, _ = PIECES[key[0]]
        xx, zz = block(key[1] + dx, key[2] + dz)
        return bg.at[xx, zz, c, pl.ds(first, size)]

    def step(what):
        key, sends = what
        if key is not None:
            if key[1:] == (0, 0):
                land(PIECES[key[0]][3])
            else:
                arrive(piece(key), piece_recv.at[KEY_ID[key]])
        for link, out in sends:
            d = 1 if link[1] == "+" else -1
            to = {"dx": d} if link[0] == "x" else {"dz": d}
            ref, n = piece(out, **to), KEY_ID[out]
            go(ref, ref, piece_send.at[n], piece_recv.at[n], device(**to))

    def share(what):
        n, (xx, zz) = BLOCK_ID[what], block(*what)
        ref = bg.at[xx, zz, c]
        go(ref, ref, share_send.at[n], share_recv.at[n], device(dc=1))

    def prepare(_):
        for load in loads[4:]:
            load.wait()
        for q in range(NX):
            wa[0, q] = wraw[:, pl.ds(q * 128, 128)] * flag(wp, q // 2)
        for k in range(NZ):
            for t in range(2):
                cols = pl.ds(t * TILE, TILE)
                ae[k, :, cols] = ae[k, :, cols] * flag(ap, 2 * k + t)

    begun = set()

    def multiply(what):
        n, (xx, zz) = BLOCK_ID[what], block(*what)
        arrive(bg.at[xx, zz, 1 - c], share_recv.at[n])
        group = GROUP[what[0]]
        fresh = group not in begun
        begun.add(group)

        def pair(p, carry):
            def part(core, t):
                start = pl.multiple_of((2 * p + t) * TILE, TILE)
                return bg[xx, zz, core, pl.ds(start, TILE), :]

            right = jnp.concatenate(
                [jnp.concatenate([part(k, 0), part(k, 1)], axis=1) for k in range(2)], axis=0
            )
            new = jnp.dot(ae[zz], right, preferred_element_type=jnp.float32)
            for t in range(2):
                new_t = new[:, t * 128 : (t + 1) * 128]
                acc[group, 2 * p + t] = new_t if fresh else acc[group, 2 * p + t] + new_t
            return carry

        lax.fori_loop(0, 2, pair, 0)

    def weights(_):
        for d in range(1, NY):
            go(wa.at[0], wa.at[NY - d], w_send.at[d - 1], w_recv.at[d - 1], device(dy=d))

    heard = []
    half = (pl.ds(0, 128), pl.ds(128, 128))

    late = []

    def rs_go(src, dst, n, d):
        copy = remote(src, dst, rs_send.at[n], rs_recv.at[n], device(dy=d))
        copy.start()
        late.append(copy)

    def scatter(dx):
        group, xx = GROUP[dx], block(dx, 0)[0]
        base = 6 * group
        rs_go(acc.at[group, 2, half[0]], rl.at[0, group], base, 1)
        rs_go(acc.at[group, 2, half[1]], rl.at[1, group], base + 1, -1)
        rs_go(acc.at[group, 1, half[1]], rs.at[0, group, half[1]], base + 2, 1)
        rs_go(acc.at[group, 3, half[0]], rs.at[1, group, half[0]], base + 3, -1)
        if not heard:
            heard.append(True)
            tot[...] = jnp.zeros_like(tot)
            for d in range(1, NY):
                arrive(wa.at[NY - d], w_recv.at[d - 1])

        def one(j, carry):
            value = acc[group, j] * wa[j, xx].astype(jnp.float32)
            tot[...] += jnp.sum(value.reshape(TILE // 8, 8, 128), axis=0)
            return carry

        lax.fori_loop(0, NY, one, 0)

    def add(dx):
        group = GROUP[dx]
        base = 6 * group
        arrive(rl.at[0, group], rs_recv.at[base])
        acc[group, 1, half[0]] += rl[0, group]
        rs_go(acc.at[group, 1, half[0]], rs.at[0, group, half[0]], base + 4, 1)
        arrive(rl.at[1, group], rs_recv.at[base + 1])
        acc[group, 3, half[1]] += rl[1, group]
        rs_go(acc.at[group, 3, half[1]], rs.at[1, group, half[1]], base + 5, -1)

    stores = []

    def store(dx):
        group, xx = GROUP[dx], block(dx, 0)[0]
        base = 6 * group
        for n, (side, part) in ((2, (0, 1)), (3, (1, 0)), (4, (0, 0)), (5, (1, 1))):
            arrive(rs.at[side, group, half[part]], rs_recv.at[base + n])
        value = acc[group, 0] + rs[0, group] + rs[1, group]
        value = value * wa[0, xx].astype(jnp.float32)
        masked[group] = value.astype(jnp.bfloat16)
        cols = pl.ds(pl.multiple_of(xx * 128, 128), 128)
        copy = pltpu.make_async_copy(masked.at[group], out_ref.at[:, cols], out_sem.at[group])
        copy.start()
        stores.append(copy)

    PEERS = {
        "y": [(d - 1, {"dy": d}) for d in range(1, NY)],
        "c": [(3, {"dc": 1})],
        "x": [(3 + d, {"dx": d}) for d in range(1, NX)],
        "z": [(6 + d, {"dz": d}) for d in range(1, NZ)],
    }

    def info_refs(stage, to, back):
        s = -1 if back else 0
        if stage == "y":
            return (iy.at[0], iy.at[to["dy"]])
        if stage == "c":
            ref = info.at[z, x, lax.rem(c + 1, 2) if back else c]
        elif stage == "x":
            ref = info.at[z, lax.rem(x + s * to["dx"] + NX, NX)]
        else:
            ref = info.at[lax.rem(z + s * to["dz"] + NZ, NZ)]
        return ref, ref

    def bits_stage(stage):
        order = "ycxz"
        if stage > 0:
            for n, to in PEERS[order[stage - 1]]:
                arrive(info_refs(order[stage - 1], to, True)[1], info_recv.at[n])
        if stage == 1:
            info[z, x, c] = iy[0] + iy[1] + iy[2] + iy[3]
        if stage < 4:
            for n, to in PEERS[order[stage]]:
                src, dst = info_refs(order[stage], to, False)
                go(src, dst, info_send.at[n], info_recv.at[n], device(**to))
            return
        at = lax.broadcasted_iota(jnp.int32, (64, 128), 0)
        lanes = lax.broadcasted_iota(jnp.int32, (64, 128), 1)
        table = jnp.zeros((64, 128), jnp.float32)
        for i in range(64):
            xi, zi, ci = i // 16, (i // 2) % 8, i % 2
            table = jnp.where(at == i, info[zi, xi, ci], table)
        tail = lanes >= 64
        bp = jnp.where(tail & (table > 1.5), 1.0, 0.0)
        wp = jnp.where(tail, table - 2.0 * bp, 0.0)
        ap = jnp.where(tail, 0.0, table).astype(jnp.bfloat16)
        wide = jnp.concatenate([bp, jnp.zeros_like(bp)], axis=0).astype(jnp.bfloat16)
        link = jnp.dot(ap, wide, preferred_element_type=jnp.float32)
        present = jnp.where(link > 0.5, wp, 0.0)
        left = (
            lax.broadcasted_iota(jnp.int32, (128, 128), 0)
            < lax.broadcasted_iota(jnp.int32, (128, 128), 1)
        )
        marks = present.astype(jnp.bfloat16)
        inside = jnp.dot(marks, jnp.where(left, 1.0, 0.0).astype(jnp.bfloat16),
                         preferred_element_type=jnp.float32)
        own = at == row
        earlier = jnp.sum(jnp.where(at < row, present, 0.0))
        before = jnp.sum(jnp.where(own, inside, 0.0), axis=0, keepdims=True) + earlier
        here = jnp.sum(jnp.where(own, present, 0.0), axis=0, keepdims=True)
        slots = jnp.where(here > 0.5, before, -1.0)
        for t in range(2):
            slot_ref[0, t] = jnp.sum(jnp.where(lane == 64 + 2 * y + t, slots, 0.0))

    SUM_AT = {"c": (0, 2, c), "y": (2, NY, y), "x": (6, NX, x), "z": (10, NZ, z)}
    SUM_ORDER = "cxzy"

    def sum_stage(k):
        if k == 0:
            value = jnp.sum(tot[...], axis=0, keepdims=True)
        else:
            base, size, me = SUM_AT[SUM_ORDER[k - 1]]
            for n, to in PEERS[SUM_ORDER[k - 1]]:
                back = lax.rem(me + size - next(iter(to.values())), size)
                arrive(ta.at[base + back], sum_recv.at[n])
            value = ta[base]
            for i in range(1, size):
                value = value + ta[base + i]
        if k == 4:
            total_ref[0, 0] = jnp.sum(value) / (TILE * math.sqrt(64 * 8))
            return
        base, _, me = SUM_AT[SUM_ORDER[k]]
        ta[base + me] = value
        for n, to in PEERS[SUM_ORDER[k]]:
            ref = ta.at[base + me]
            go(ref, ref, sum_send.at[n], sum_recv.at[n], device(**to))
        if k == 1:
            finish()

    def finish():
        while sent:
            sent.pop(0).wait_send()

    run = {
        "step": step, "share": share, "prepare": prepare, "multiply": multiply,
        "weights": weights, "scatter": scatter, "add": add, "store": store,
        "bits": bits_stage, "sum": sum_stage,
    }
    for kind, what in program():
        run[kind](what)
    finish()
    for copy in late:
        copy.wait_send()
    for copy in stores:
        copy.wait()
    for d in (1, 2, 3):
        move(d).wait_send()

    @pl.when(jnp.logical_not(diagonal))
    def _():
        move(0).wait_send()


def on_device(a_values, a_present, b_values, b_present, w_values, w_present):
    hbm = pl.BlockSpec(memory_space=pltpu.HBM)
    smem = pl.BlockSpec(memory_space=pltpu.SMEM)
    dma = pltpu.SemaphoreType.DMA
    bf16, f32, i32 = jnp.bfloat16, jnp.float32, jnp.int32
    masked, slot, total = pl.pallas_call(
        kernel,
        out_shape=(
            jax.ShapeDtypeStruct((TILE, 512), bf16),
            jax.ShapeDtypeStruct((1, 2), f32),
            jax.ShapeDtypeStruct((1, 1), f32),
        ),
        in_specs=[hbm] * 6,
        out_specs=(hbm, smem, smem),
        scratch_shapes=[
            pltpu.VMEM((NX, NZ, 2, 1024, 128), bf16),
            pltpu.VMEM((NZ, TILE, 2 * TILE), bf16),
            pltpu.VMEM((NX, NY, TILE, 128), f32),
            pltpu.VMEM((2, NX, 128, 128), f32),
            pltpu.VMEM((2, NX, TILE, 128), f32),
            pltpu.VMEM((NY, NX, TILE, 128), bf16),
            pltpu.VMEM((NX, TILE, 128), bf16),
            pltpu.VMEM((TILE, 512), bf16),
            pltpu.VMEM((TILE, 512), bf16),
            pltpu.VMEM((NX, TILE, 128), bf16),
            pltpu.VMEM((8, 128), f32),
            pltpu.VMEM((NY, 1, 128), f32),
            pltpu.VMEM((NZ, NX, 2, 1, 128), f32),
            pltpu.VMEM((18, 1, 128), f32),
            pltpu.SMEM((1, 16), i32),
            pltpu.SMEM((1, 2), i32),
            pltpu.SMEM((1, 2), i32),
            dma((NZ,)), dma((5,)), dma((NX,)), dma((NX,)), dma((NY,)),
            dma((len(KEY_ID),)), dma((len(KEY_ID),)),
            dma((len(BLOCKS),)), dma((len(BLOCKS),)),
            dma((3,)), dma((3,)), dma((24,)), dma((24,)),
            dma((14,)), dma((14,)), dma((14,)), dma((14,)),
        ],
        compiler_params=pltpu.CompilerParams(
            collective_id=0, has_side_effects=True, vmem_limit_bytes=60 * 2**20
        ),
    )(a_values, a_present, b_values, b_present, w_values, w_present)
    return masked, slot, total.reshape(())


def solution(mesh):
    spec = P("row", "col")
    return jax.shard_map(
        on_device, mesh=mesh, in_specs=(spec,) * 6, out_specs=(spec, spec, P()),
        check_vma=False,
    )
```

```python
import heapq
import math

import jax
import jax.numpy as jnp
from jax import lax
from jax.experimental import pallas as pl
from jax.experimental.pallas import tpu as pltpu
from jax.sharding import PartitionSpec as P

MESH = pl.DeviceIdType.MESH
TILE = 256
NX, NZ, NY = 4, 8, 4
LINKS = ("x+", "x-", "z+", "z-")
PIECES = (
    (True, 0, 256, 0),
    (True, 256, 256, 1),
    (True, 768, 128, 3),
    (False, 512, 256, 2),
    (False, 896, 128, 3),
)
BLOCKS = [(dx, dz) for dx in (0, -1, 1, 2) for dz in (0, -1, 1, -2, 2, -3, 3, 4)]
BLOCK_ID = {block: n for n, block in enumerate(BLOCKS)}
GROUP = {0: 0, -1: 1, 1: 2, 2: 3}
KEY_ID = {
    key: n for n, key in enumerate((p, *block) for p in range(len(PIECES)) for block in BLOCKS[1:])
}
MOVED = NX * NZ - 1
LATENCY, RATE, LEAD = 2.8, 46.6e3, 2.0
STEP, ISSUE, MULTIPLY, SHARE = 0.03, 0.02, 0.47, 1.5
READY = (0.0, 0.8, 0.8, 1.2, 0.8)
X_FIRST_RANK = (0, 1, 2)
X_RANK = (1, 2)
BITS = (1.0, 12.0, 30.0)
SUMS = (0.0, 4.2, 4.2)


def program():
    free = dict.fromkeys(LINKS + ("y+", "y-"), 0.0)
    waiting = {link: [] for link in LINKS}
    inbox, ready, items, count = [], [], [], [0]
    missing = {block: len(PIECES) for block in BLOCKS}
    left = {dx: NZ for dx in GROUP}

    def push(heap, when, what):
        count[0] += 1
        heapq.heappush(heap, (when, count[0], what))

    def commit(now):
        sends = []
        for link in LINKS:
            while waiting[link] and free[link] - now < LEAD:
                key = heapq.heappop(waiting[link])[2]
                free[link] = max(now, free[link]) + PIECES[key[0]][2] * 256 / RATE
                push(inbox, free[link] + LATENCY, key)
                sends.append((link, key))
        return tuple(sends)

    def along_y(link, now, rows):
        free[link] = max(now, free[link]) + rows * 512 / RATE
        return free[link] + LATENCY

    def along_z(p, dx, dz):
        rank = -1 if PIECES[p][0] else X_FIRST_RANK[abs(dx)]
        if dz == 0:
            push(waiting["z+"], rank, (p, dx, -1))
            push(waiting["z-"], rank, (p, dx, 1))
        elif abs(dz) < 3:
            sign = 1 if dz > 0 else -1
            push(waiting["z-" if dz > 0 else "z+"], rank, (p, dx, dz + sign))
        elif abs(dz) == 3:
            sign = -1 if (p + abs(dx) // 2 + (dx == 1)) % 2 == 0 else 1
            if (dz < 0) == (sign < 0):
                push(waiting["z-" if dz > 0 else "z+"], rank, (p, dx, 4))

    def along_x(p, dx, dz):
        if dx == 0:
            rank = X_RANK[0] if PIECES[p][0] else -1
            push(waiting["x+"], rank, (p, -1, dz))
            push(waiting["x-"], rank, (p, 1, dz))
        elif dx == (-1 if (p + dz) % 2 == 0 else 1):
            rank = X_RANK[1] if PIECES[p][0] else 0
            push(waiting["x+" if dx < 0 else "x-"], rank, (p, 2, dz))

    for p, when in enumerate(READY):
        push(inbox, when, (p, 0, 0))
    for stage, when in enumerate(BITS):
        push(ready, when, ("bits", stage))
    push(ready, 3.0, ("weights", None))
    push(ready, 2.5, ("prepare", None))
    now, stage = 0.0, 0
    while inbox or ready:
        if inbox and inbox[0][0] <= now:
            key = heapq.heappop(inbox)[2]
            p, dx, dz = key
            if PIECES[p][0]:
                if dx == 0:
                    along_z(*key)
                along_x(*key)
            else:
                if dz == 0:
                    along_x(*key)
                along_z(*key)
            now += STEP
            sends = commit(now)
            now += ISSUE * len(sends)
            items.append(("step", (key, sends)))
            block = dx, dz
            missing[block] -= 1
            if missing[block] == 0:
                items.append(("share", block))
                push(ready, now + SHARE, ("multiply", block))
        elif ready and ready[0][0] <= now:
            kind, what = heapq.heappop(ready)[2]
            items.append((kind, what))
            if kind == "multiply":
                now += MULTIPLY
                dx = what[0]
                left[dx] -= 1
                if left[dx] == 0:
                    items.append(("scatter", dx))
                    now += 0.25
                    first = max(along_y("y+", now, 128), along_y("y-", now, 128))
                    along_y("y+", now, 128), along_y("y-", now, 128)
                    push(ready, first, ("add", dx))
                    if not any(left.values()):
                        push(ready, now, ("sum", 0))
            elif kind == "add":
                now += 0.15
                last = max(along_y("y+", now, 128), along_y("y-", now, 128))
                push(ready, last, ("store", what))
            elif kind == "sum" and what < 2:
                push(ready, now + SUMS[what + 1], ("sum", what + 1))
            elif kind == "prepare":
                now += 0.3
            elif kind == "store":
                now += 0.1
            sends = commit(now)
            if sends:
                items.append(("step", (None, sends)))
        else:
            now = min(heap[0][0] for heap in (inbox, ready) if heap)
    program.end = now
    return items


def kernel(
    a_ref, ap_ref, b_ref, bp_ref, w_ref, wp_ref,
    out_ref, slot_ref, total_ref,
    bg, ae, acc, rl, rs, wa, bm, braw, wraw, masked, slots_v, tot, ixy, info, ta, ap, bp, wp,
    a_sem, in_sem, out_sem, move_send, move_recv, bulk_send, piece_recv, share_recv,
    w_send, w_recv, rs_send, rl_recv, rs_recv, info_send, info_recv, sum_send, sum_recv,
):
    row, y = lax.axis_index("row"), lax.axis_index("col")
    c = lax.rem(row, 2)
    z = lax.rem(row // 2, NZ)
    x = row // (2 * NZ)

    def device(dx=0, dy=0, dz=0, dc=0):
        xx, zz = lax.rem(x + dx + NX, NX), lax.rem(z + dz + NZ, NZ)
        return ((xx * NZ + zz) * 2 + lax.rem(c + dc, 2), lax.rem(y + dy + NY, NY))

    def place(xx, yy):
        return ((xx * NZ + z) * 2 + c, yy)

    def remote(src, dst, send, recv, to):
        return pltpu.make_async_remote_copy(
            src_ref=src, dst_ref=dst, send_sem=send, recv_sem=recv,
            device_id=to, device_id_type=MESH,
        )

    def arrive(dst, recv):
        remote(dst, dst, sum_send, recv, device(dc=1)).wait_recv()

    def gone(src, send):
        remote(src, src, send, sum_recv.at[0], device(dc=1)).wait_send()

    def go(*args):
        remote(*args).start()

    def at(xx, zz, core, first=0, size=1024):
        start = ((xx * NZ + zz) * 2 + core) * 1024 + first
        return pl.ds(pl.multiple_of(start, 16), size)

    ZC = [{"dz": d, "dc": e} for d in range(NZ) for e in range(2)][1:]
    XY = [{"dx": d, "dy": e} for d in range(NX) for e in range(NY)][1:]

    loads = [
        pltpu.make_async_copy(src, dst, in_sem.at[n])
        for n, (src, dst) in enumerate(
            ((b_ref, braw), (bp_ref, bp), (ap_ref, ap), (wp_ref, wp), (w_ref, wraw))
        )
    ]
    for k in range(NZ):
        loads.append(pltpu.make_async_copy(
            a_ref.at[:, pl.ds(k * 2 * TILE, 2 * TILE)], ae.at[k], a_sem
        ))
    for load in loads:
        load.start()
    barrier = pltpu.get_barrier_semaphore()

    def greet(to):
        pl.semaphore_signal(barrier, inc=1, device_id=to, device_id_type=MESH)

    for to in ZC + XY:
        greet(device(**to))

    def flag(ref, n):
        return ref[0, n].astype(jnp.float32).astype(jnp.bfloat16)

    for load in loads[:2]:
        load.wait()
    for q in range(NX):
        bm[q] = braw[:, pl.ds(q * 128, 128)] * flag(bp, q // 2)
    for load in loads[2:4]:
        load.wait()
    lane = lax.broadcasted_iota(jnp.int32, (1, 128), 1)
    bits = jnp.zeros((1, 128), jnp.float32)
    for t in range(16):
        bits = jnp.where(lane == 16 * y + t, ap[0, t].astype(jnp.float32), bits)
    for t in range(2):
        both = wp[0, t] + 2 * bp[0, t]
        bits = jnp.where(lane == 64 + 2 * y + t, both.astype(jnp.float32), bits)
    ixy[x * NY + y] = bits
    pl.semaphore_wait(barrier, len(ZC + XY))

    diagonal = x == y
    mine = lax.rem(y - x + NY, NY)

    def move(d):
        q = lax.rem(x + d, NX)
        dst = bg.at[at(q, z, c, mine * TILE, TILE)]
        return remote(bm.at[q], dst, move_send.at[d], move_recv.at[mine], place(q, x))

    for d in (2, 1, 3):
        move(d).start()

    @pl.when(jnp.logical_not(diagonal))
    def _():
        move(0).start()

    @pl.when(diagonal)
    def _():
        bg[at(x, z, c, mine * TILE, TILE)] = bm[x]

    landed = set()

    def land(j):
        if j in landed:
            return
        landed.add(j)
        dst = bg.at[at(x, z, c, j * TILE, TILE)]
        if j > 0:
            arrive(dst, move_recv.at[j])
            return

        @pl.when(jnp.logical_not(diagonal))
        def _():
            arrive(dst, move_recv.at[0])

    def block(dx, dz):
        return lax.rem(x + dx + NX, NX), lax.rem(z + dz + NZ, NZ)

    def piece(key, dx=0, dz=0):
        _, first, size, _ = PIECES[key[0]]
        xx, zz = block(key[1] + dx, key[2] + dz)
        return bg.at[at(xx, zz, c, first, size)]

    def step(what):
        key, sends = what
        if key is not None:
            if key[1:] == (0, 0):
                land(PIECES[key[0]][3])
            else:
                arrive(piece(key), piece_recv.at[KEY_ID[key]])
        for link, out in sends:
            d = 1 if link[1] == "+" else -1
            to = {"dx": d} if link[0] == "x" else {"dz": d}
            ref, n = piece(out, **to), KEY_ID[out]
            go(ref, ref, bulk_send, piece_recv.at[n], device(**to))

    def share(what):
        n, (xx, zz) = BLOCK_ID[what], block(*what)
        ref = bg.at[at(xx, zz, c)]
        go(ref, ref, bulk_send, share_recv.at[n], device(dc=1))

    def prepare(_):
        loads[4].wait()
        pltpu.make_async_copy(ae, ae, a_sem).wait()
        for q in range(NX):
            wa[0, q] = wraw[:, pl.ds(q * 128, 128)] * flag(wp, q // 2)
        for k in range(NZ):
            for t in range(2):
                cols = pl.ds(t * TILE, TILE)
                ae[k, :, cols] = ae[k, :, cols] * flag(ap, 2 * k + t)

    begun = set()

    def multiply(what):
        n, (xx, zz) = BLOCK_ID[what], block(*what)
        arrive(bg.at[at(xx, zz, 1 - c)], share_recv.at[n])
        group = GROUP[what[0]]
        fresh = group not in begun
        begun.add(group)

        def pair(p, carry):
            def part(core, t):
                return bg[at(xx, zz, core, (2 * p + t) * TILE, TILE), :]

            right = jnp.concatenate(
                [jnp.concatenate([part(k, 0), part(k, 1)], axis=1) for k in range(2)], axis=0
            )
            new = jnp.dot(ae[zz], right, preferred_element_type=jnp.float32)
            for t in range(2):
                new_t = new[:, t * 128 : (t + 1) * 128]
                acc[group, 2 * p + t] = new_t if fresh else acc[group, 2 * p + t] + new_t
            return carry

        lax.fori_loop(0, 2, pair, 0)

    def weights(_):
        for d in range(1, NY):
            go(wa.at[0], wa.at[NY - d], w_send, w_recv, device(dy=d))

    heard = []
    half = (pl.ds(0, 128), pl.ds(128, 128))

    def scatter(dx):
        group, xx = GROUP[dx], block(dx, 0)[0]
        for d, src, dst, recv in (
            (1, acc.at[group, 2, half[0]], rl.at[group, 0], rl_recv),
            (-1, acc.at[group, 2, half[1]], rl.at[group, 1], rl_recv),
            (1, acc.at[group, 1, half[1]], rs.at[group, 0, half[1]], rs_recv),
            (-1, acc.at[group, 3, half[0]], rs.at[group, 1, half[0]], rs_recv),
        ):
            go(src, dst, rs_send, recv.at[group], device(dy=d))
        if not heard:
            heard.append(True)
            tot[...] = jnp.zeros_like(tot)
            arrive(wa.at[pl.ds(1, NY - 1)], w_recv)

        def one(j, carry):
            value = acc[group, j] * wa[j, xx].astype(jnp.float32)
            tot[...] += jnp.sum(value.reshape(TILE // 8, 8, 128), axis=0)
            return carry

        lax.fori_loop(0, NY, one, 0)

    def add(dx):
        group = GROUP[dx]
        arrive(rl.at[group], rl_recv.at[group])
        acc[group, 1, half[0]] += rl[group, 0]
        acc[group, 3, half[1]] += rl[group, 1]
        for d, tile, side, part in ((1, 1, 0, 0), (-1, 3, 1, 1)):
            src, dst = acc.at[group, tile, half[part]], rs.at[group, side, half[part]]
            go(src, dst, rs_send, rs_recv.at[group], device(dy=d))

    outs = []

    def put(src, dst, n):
        copy = pltpu.make_async_copy(src, dst, out_sem.at[n])
        copy.start()
        outs.append(copy)

    def store(dx):
        group, xx = GROUP[dx], block(dx, 0)[0]
        arrive(rs.at[group], rs_recv.at[group])
        value = acc[group, 0] + rs[group, 0] + rs[group, 1]
        value = value * wa[0, xx].astype(jnp.float32)
        cols = pl.ds(pl.multiple_of(xx * 128, 128), 128)
        masked[group] = value.astype(jnp.bfloat16)
        put(masked.at[group], out_ref.at[:, cols], group)

    def bits_stage(stage):
        if stage == 0:
            for to in XY:
                ref = ixy.at[x * NY + y]
                go(ref, ref, info_send.at[0], info_recv.at[0], device(**to))
            return
        if stage == 1:
            arrive(ixy.at[pl.ds(0, len(XY))], info_recv.at[0])
            rows = pl.ds((z * 2 + c) * NX, NX)
            for k in range(NX):
                line = [ixy[k * NY + n] for n in range(NY)]
                info[(z * 2 + c) * NX + k] = line[0] + line[1] + line[2] + line[3]
            for to in ZC:
                go(info.at[rows], info.at[rows], info_send.at[1], info_recv.at[1], device(**to))
            return
        arrive(info.at[pl.ds(0, NX * len(ZC))], info_recv.at[1])
        line = lax.broadcasted_iota(jnp.int32, (64, 128), 0)
        lanes = lax.broadcasted_iota(jnp.int32, (64, 128), 1)
        table = jnp.zeros((64, 128), jnp.float32)
        for i in range(64):
            xi, zi, ci = i // 16, (i // 2) % 8, i % 2
            table = jnp.where(line == i, info[(zi * 2 + ci) * NX + xi], table)
        tail = lanes >= 64
        bp = jnp.where(tail & (table > 1.5), 1.0, 0.0)
        wp = jnp.where(tail, table - 2.0 * bp, 0.0)
        ap = jnp.where(tail, 0.0, table).astype(jnp.bfloat16)
        wide = jnp.concatenate([bp, jnp.zeros_like(bp)], axis=0).astype(jnp.bfloat16)
        link = jnp.dot(ap, wide, preferred_element_type=jnp.float32)
        present = jnp.where(link > 0.5, wp, 0.0)
        left = (
            lax.broadcasted_iota(jnp.int32, (128, 128), 0)
            < lax.broadcasted_iota(jnp.int32, (128, 128), 1)
        )
        marks = present.astype(jnp.bfloat16)
        inside = jnp.dot(marks, jnp.where(left, 1.0, 0.0).astype(jnp.bfloat16),
                         preferred_element_type=jnp.float32)
        own = line == row
        earlier = jnp.sum(jnp.where(line < row, present, 0.0))
        before = jnp.sum(jnp.where(own, inside, 0.0), axis=0, keepdims=True) + earlier
        here = jnp.sum(jnp.where(own, present, 0.0), axis=0, keepdims=True)
        slots = jnp.where(here > 0.5, before, -1.0)
        for t in range(2):
            here = jnp.where(lane == 64 + 2 * y + t, slots, 0.0)
            slots_v[:, pl.ds(t, 1)] = jnp.sum(here, axis=1, keepdims=True)
        put(slots_v, slot_ref, 4)

    def sum_stage(k):
        if k == 0:
            value = jnp.sum(tot[...], axis=0, keepdims=True)
            first, size, mine, peers = 0, 16, z * 2 + c, ZC
        else:
            arrive(ta.at[pl.ds(16 * (k - 1), 15)], sum_recv.at[k - 1])
            value = ta[16 * (k - 1)]
            for n in range(1, 16):
                value = value + ta[16 * (k - 1) + n]
            first, size, mine, peers = 16, 16, x * NY + y, XY
        if k == 2:
            total_ref[0, 0] = jnp.sum(value) / (TILE * math.sqrt(64 * 8))
            return
        ta[first + mine] = value
        for to in peers:
            ref = ta.at[first + mine]
            go(ref, ref, sum_send, sum_recv.at[k], device(**to))

    run = {
        "step": step, "share": share, "prepare": prepare, "multiply": multiply,
        "weights": weights, "scatter": scatter, "add": add, "store": store,
        "bits": bits_stage, "sum": sum_stage,
    }
    for kind, what in program():
        run[kind](what)
    gone(bg.at[pl.ds(0, (2 * MOVED + 1) * 1024)], bulk_send)
    gone(acc.at[pl.ds(0, 3)], rs_send)
    gone(wa.at[pl.ds(0, 3)], w_send)
    gone(ixy.at[pl.ds(0, 15)], info_send.at[0])
    gone(info.at[pl.ds(0, 60)], info_send.at[1])
    gone(ta.at[pl.ds(0, 30)], sum_send)
    for copy in outs:
        copy.wait()
    for d in (1, 2, 3):
        move(d).wait_send()

    @pl.when(jnp.logical_not(diagonal))
    def _():
        move(0).wait_send()


def on_device(a_values, a_present, b_values, b_present, w_values, w_present):
    hbm = pl.BlockSpec(memory_space=pltpu.HBM)
    smem = pl.BlockSpec(memory_space=pltpu.SMEM)
    dma = pltpu.SemaphoreType.DMA
    bf16, f32, i32 = jnp.bfloat16, jnp.float32, jnp.int32
    masked, slot, total = pl.pallas_call(
        kernel,
        out_shape=(
            jax.ShapeDtypeStruct((TILE, 512), bf16),
            jax.ShapeDtypeStruct((1, 2), f32),
            jax.ShapeDtypeStruct((1, 1), f32),
        ),
        in_specs=[hbm] * 6,
        out_specs=(hbm, hbm, smem),
        scratch_shapes=[
            pltpu.VMEM((NX * NZ * 2 * 1024, 128), bf16),
            pltpu.VMEM((NZ, TILE, 2 * TILE), bf16),
            pltpu.VMEM((NX, NY, TILE, 128), f32),
            pltpu.VMEM((NX, 2, 128, 128), f32),
            pltpu.VMEM((NX, 2, TILE, 128), f32),
            pltpu.VMEM((NY, NX, TILE, 128), bf16),
            pltpu.VMEM((NX, TILE, 128), bf16),
            pltpu.VMEM((TILE, 512), bf16),
            pltpu.VMEM((TILE, 512), bf16),
            pltpu.VMEM((NX, TILE, 128), bf16),
            pltpu.VMEM((1, 2), f32),
            pltpu.VMEM((8, 128), f32),
            pltpu.VMEM((NX * NY, 1, 128), f32),
            pltpu.VMEM((64, 1, 128), f32),
            pltpu.VMEM((32, 1, 128), f32),
            pltpu.SMEM((1, 16), i32),
            pltpu.SMEM((1, 2), i32),
            pltpu.SMEM((1, 2), i32),
            dma, dma((5,)), dma((5,)), dma((NX,)), dma((NY,)),
            dma, dma((len(KEY_ID),)), dma((len(BLOCKS),)),
            dma, dma, dma, dma((NX,)), dma((NX,)),
            dma((2,)), dma((2,)), dma, dma((2,)),
        ],
        compiler_params=pltpu.CompilerParams(
            collective_id=0, has_side_effects=True, vmem_limit_bytes=60 * 2**20
        ),
    )(a_values, a_present, b_values, b_present, w_values, w_present)
    return masked, slot, total.reshape(())


def solution(mesh):
    spec = P("row", "col")
    return jax.shard_map(
        on_device, mesh=mesh, in_specs=(spec,) * 6, out_specs=(spec, spec, P()),
        check_vma=False,
    )
```

```python
import heapq
import math

import jax
import jax.numpy as jnp
from jax import lax
from jax.experimental import pallas as pl
from jax.experimental.pallas import tpu as pltpu
from jax.sharding import PartitionSpec as P

MESH = pl.DeviceIdType.MESH
TILE = 256
NX, NZ, NY = 4, 8, 4
LINKS = ("x+", "x-", "z+", "z-")
PIECES = (
    ("Z", 0, 256, (0,)),
    ("Z", 256, 352, (1, 2)),
    ("X", 608, 416, (2, 3)),
    ("J", 0, 608, ()),
)
JOINED = len(PIECES) - 1
BLOCKS = [(dx, dz) for dx in (0, -1, 1, 2) for dz in (0, -1, 1, -2, 2, -3, 3, 4)]
BLOCK_ID = {block: n for n, block in enumerate(BLOCKS)}
GROUP = {0: 0, -1: 1, 1: 2, 2: 3}
KEYS = [
    (p, *block)
    for p in range(len(PIECES))
    for block in BLOCKS[1:]
    if {"Z": block[0] == 0, "X": True, "J": block[0] != 0}[PIECES[p][0]]
]
KEY_ID = {key: n for n, key in enumerate(KEYS)}
MOVED = NX * NZ - 1
LATENCY, Y_LATENCY, RATE, LEAD = 2.5, 3.0, 46.6e3, 1.85
STEP, MULTIPLY, SHARE = 0.03, 0.47, 1.5
READY = (0.0, 0.8, 1.2)
BITS = (1.0, 12.0, 30.0)
SUM = 3.8


def rank_z(p, dx, dz):
    return -1.0 if PIECES[p][0] == "Z" else abs(dx) - 0.6 * abs(dz)


def rank_x(p, dx):
    return {"X": (-1.0, 0.0), "J": (1.0, 2.0)}[PIECES[p][0]][abs(dx)]


def program():
    free = dict.fromkeys(LINKS + ("y+", "y-"), 0.0)
    waiting = {link: [] for link in LINKS}
    inbox, ready, items, count = [], [], [], [0]
    missing = {block: 2 if block[0] else len(PIECES) - 1 for block in BLOCKS}
    unjoined = {dz: 2 for dx, dz in BLOCKS if dx == 0}
    left = {dx: NZ for dx in GROUP}

    def push(heap, when, what):
        count[0] += 1
        heapq.heappush(heap, (when, count[0], what))

    def commit(now):
        sends = []
        for link in LINKS:
            while waiting[link] and free[link] - now < LEAD:
                key = heapq.heappop(waiting[link])[2]
                free[link] = max(now, free[link]) + PIECES[key[0]][2] * 256 / RATE
                push(inbox, free[link] + LATENCY, key)
                sends.append((link, key))
        return tuple(sends)

    def along_y(link, now, rows):
        free[link] = max(now, free[link]) + rows * 512 / RATE
        return free[link] + Y_LATENCY

    def along_z(p, dx, dz):
        rank = rank_z(p, dx, dz)
        if dz == 0:
            push(waiting["z+"], rank, (p, dx, -1))
            push(waiting["z-"], rank, (p, dx, 1))
        elif abs(dz) < 3:
            sign = 1 if dz > 0 else -1
            push(waiting["z-" if dz > 0 else "z+"], rank, (p, dx, dz + sign))
        elif abs(dz) == 3:
            sign = -1 if (p + abs(dx) // 2 + (dx == 1)) % 2 == 0 else 1
            if (dz < 0) == (sign < 0):
                push(waiting["z-" if dz > 0 else "z+"], rank, (p, dx, 4))

    def along_x(p, dx, dz):
        rank = rank_x(p, dx) if abs(dx) < 2 else 0.0
        if dx == 0:
            push(waiting["x+"], rank, (p, -1, dz))
            push(waiting["x-"], rank, (p, 1, dz))
        elif dx == (-1 if (p + dz) % 2 == 0 else 1):
            push(waiting["x+" if dx < 0 else "x-"], rank, (p, 2, dz))

    for p, when in enumerate(READY):
        push(inbox, when, (p, 0, 0))
    for stage, when in enumerate(BITS):
        push(ready, when, ("bits", stage))
    push(ready, 3.0, ("weights", None))
    push(ready, 2.5, ("prepare", None))
    now = 0.0
    while inbox or ready:
        if inbox and inbox[0][0] <= now:
            key = heapq.heappop(inbox)[2]
            p, dx, dz = key
            if PIECES[p][0] == "Z":
                along_z(*key)
                unjoined[dz] -= 1
                if unjoined[dz] == 0:
                    along_x(JOINED, 0, dz)
            elif PIECES[p][0] == "J":
                along_x(*key)
            else:
                if dz == 0:
                    along_x(*key)
                along_z(*key)
            now += STEP
            sends = commit(now)
            items.append(("step", (key, sends)))
            block = dx, dz
            missing[block] -= 1
            if missing[block] == 0:
                items.append(("share", block))
                push(ready, now + SHARE, ("multiply", block))
        elif ready and ready[0][0] <= now:
            kind, what = heapq.heappop(ready)[2]
            items.append((kind, what))
            if kind == "multiply":
                now += MULTIPLY
                dx = what[0]
                left[dx] -= 1
                if left[dx] == 0:
                    items.append(("scatter", dx))
                    now += 0.25
                    first = max(along_y("y+", now, 128), along_y("y-", now, 128))
                    along_y("y+", now, 128), along_y("y-", now, 128)
                    push(ready, first, ("add", dx))
                    if not any(left.values()):
                        push(ready, now, ("sum", 0))
            elif kind == "add":
                now += 0.15
                last = max(along_y("y+", now, 128), along_y("y-", now, 128))
                push(ready, last, ("store", what))
            elif kind == "sum" and what < 2:
                push(ready, now + SUM, ("sum", what + 1))
            elif kind == "prepare":
                now += 0.3
            elif kind == "store":
                now += 0.1
            sends = commit(now)
            if sends:
                items.append(("step", (None, sends)))
        else:
            now = min(heap[0][0] for heap in (inbox, ready) if heap)
    return items


def kernel(
    a_ref, ap_ref, b_ref, bp_ref, w_ref, wp_ref,
    out_ref, slot_ref, total_ref,
    bg, ae, acc, rl, rs, wa, bm, braw, wraw, masked, slots_v, tot, ixy, info, ta, ap, bp, wp,
    a_sem, in_sem, out_sem, move_send, move_recv, bulk_send, piece_recv, share_recv,
    w_send, w_recv, rs_send, rl_recv, rs_recv, info_send, info_recv, sum_send, sum_recv,
):
    row, y = lax.axis_index("row"), lax.axis_index("col")
    c = lax.rem(row, 2)
    z = lax.rem(row // 2, NZ)
    x = row // (2 * NZ)

    def device(dx=0, dy=0, dz=0, dc=0):
        xx, zz = lax.rem(x + dx + NX, NX), lax.rem(z + dz + NZ, NZ)
        return ((xx * NZ + zz) * 2 + lax.rem(c + dc, 2), lax.rem(y + dy + NY, NY))

    def place(xx, yy):
        return ((xx * NZ + z) * 2 + c, yy)

    def remote(src, dst, send, recv, to):
        return pltpu.make_async_remote_copy(
            src_ref=src, dst_ref=dst, send_sem=send, recv_sem=recv,
            device_id=to, device_id_type=MESH,
        )

    def arrive(dst, recv):
        remote(dst, dst, sum_send, recv, device(dc=1)).wait_recv()

    def gone(src, send):
        remote(src, src, send, sum_recv.at[0], device(dc=1)).wait_send()

    def go(*args):
        remote(*args).start()

    def at(xx, zz, core, first=0, size=1024):
        start = ((xx * NZ + zz) * 2 + core) * 1024 + first
        return pl.ds(pl.multiple_of(start, 16), size)

    ZC = [{"dz": d, "dc": e} for d in range(NZ) for e in range(2)][1:]
    XY = [{"dx": d, "dy": e} for d in range(NX) for e in range(NY)][1:]

    loads = [
        pltpu.make_async_copy(src, dst, in_sem.at[n])
        for n, (src, dst) in enumerate(
            ((b_ref, braw), (bp_ref, bp), (ap_ref, ap), (wp_ref, wp), (w_ref, wraw))
        )
    ]
    for k in range(NZ):
        loads.append(pltpu.make_async_copy(
            a_ref.at[:, pl.ds(k * 2 * TILE, 2 * TILE)], ae.at[k], a_sem
        ))
    for load in loads:
        load.start()
    barrier = pltpu.get_barrier_semaphore()

    def greet(to):
        pl.semaphore_signal(barrier, inc=1, device_id=to, device_id_type=MESH)

    for to in ZC + XY:
        greet(device(**to))

    def flag(ref, n):
        return ref[0, n].astype(jnp.float32).astype(jnp.bfloat16)

    for load in loads[:2]:
        load.wait()
    for q in range(NX):
        bm[q] = braw[:, pl.ds(q * 128, 128)] * flag(bp, q // 2)
    for load in loads[2:4]:
        load.wait()
    lane = lax.broadcasted_iota(jnp.int32, (1, 128), 1)
    bits = jnp.zeros((1, 128), jnp.float32)
    for t in range(16):
        bits = jnp.where(lane == 16 * y + t, ap[0, t].astype(jnp.float32), bits)
    for t in range(2):
        both = wp[0, t] + 2 * bp[0, t]
        bits = jnp.where(lane == 64 + 2 * y + t, both.astype(jnp.float32), bits)
    ixy[x * NY + y] = bits
    pl.semaphore_wait(barrier, len(ZC + XY))

    diagonal = x == y
    mine = lax.rem(y - x + NY, NY)

    def move(d):
        q = lax.rem(x + d, NX)
        dst = bg.at[at(q, z, c, mine * TILE, TILE)]
        return remote(bm.at[q], dst, move_send.at[d], move_recv.at[mine], place(q, x))

    for d in (2, 1, 3):
        move(d).start()

    @pl.when(jnp.logical_not(diagonal))
    def _():
        move(0).start()

    @pl.when(diagonal)
    def _():
        bg[at(x, z, c, mine * TILE, TILE)] = bm[x]

    landed = set()

    def land(j):
        if j in landed:
            return
        landed.add(j)
        dst = bg.at[at(x, z, c, j * TILE, TILE)]
        if j > 0:
            arrive(dst, move_recv.at[j])
            return

        @pl.when(jnp.logical_not(diagonal))
        def _():
            arrive(dst, move_recv.at[0])

    def block(dx, dz):
        return lax.rem(x + dx + NX, NX), lax.rem(z + dz + NZ, NZ)

    def piece(key, dx=0, dz=0):
        _, first, size, _ = PIECES[key[0]]
        xx, zz = block(key[1] + dx, key[2] + dz)
        return bg.at[at(xx, zz, c, first, size)]

    def step(what):
        key, sends = what
        if key is not None:
            if key[1:] == (0, 0):
                for tile in PIECES[key[0]][3]:
                    land(tile)
            else:
                arrive(piece(key), piece_recv.at[KEY_ID[key]])
        for link, out in sends:
            d = 1 if link[1] == "+" else -1
            to = {"dx": d} if link[0] == "x" else {"dz": d}
            ref, n = piece(out, **to), KEY_ID[out]
            go(ref, ref, bulk_send, piece_recv.at[n], device(**to))

    def share(what):
        n, (xx, zz) = BLOCK_ID[what], block(*what)
        ref = bg.at[at(xx, zz, c)]
        go(ref, ref, bulk_send, share_recv.at[n], device(dc=1))

    def prepare(_):
        loads[4].wait()
        pltpu.make_async_copy(ae, ae, a_sem).wait()
        for q in range(NX):
            wa[0, q] = wraw[:, pl.ds(q * 128, 128)] * flag(wp, q // 2)
        for k in range(NZ):
            for t in range(2):
                cols = pl.ds(t * TILE, TILE)
                ae[k, :, cols] = ae[k, :, cols] * flag(ap, 2 * k + t)

    begun = set()

    def multiply(what):
        n, (xx, zz) = BLOCK_ID[what], block(*what)
        arrive(bg.at[at(xx, zz, 1 - c)], share_recv.at[n])
        group = GROUP[what[0]]
        fresh = group not in begun
        begun.add(group)

        for p in range(2):

            def part(core, t):
                return bg[at(xx, zz, core, (2 * p + t) * TILE, TILE), :]

            right = jnp.concatenate(
                [jnp.concatenate([part(k, 0), part(k, 1)], axis=1) for k in range(2)], axis=0
            )
            new = jnp.dot(ae[zz], right, preferred_element_type=jnp.float32)
            for t in range(2):
                new_t = new[:, t * 128 : (t + 1) * 128]
                acc[group, 2 * p + t] = new_t if fresh else acc[group, 2 * p + t] + new_t

    def weights(_):
        for d in range(1, NY):
            go(wa.at[0], wa.at[NY - d], w_send, w_recv, device(dy=d))

    heard = []
    half = (pl.ds(0, 128), pl.ds(128, 128))

    def scatter(dx):
        group, xx = GROUP[dx], block(dx, 0)[0]
        for d, src, dst, recv in (
            (1, acc.at[group, 2, half[0]], rl.at[group, 0], rl_recv),
            (-1, acc.at[group, 2, half[1]], rl.at[group, 1], rl_recv),
            (1, acc.at[group, 1, half[1]], rs.at[group, 0, half[1]], rs_recv),
            (-1, acc.at[group, 3, half[0]], rs.at[group, 1, half[0]], rs_recv),
        ):
            go(src, dst, rs_send, recv.at[group], device(dy=d))
        if not heard:
            heard.append(True)
            tot[...] = jnp.zeros_like(tot)
            arrive(wa.at[pl.ds(1, NY - 1)], w_recv)

        def one(j, carry):
            value = acc[group, j] * wa[j, xx].astype(jnp.float32)
            tot[...] += jnp.sum(value.reshape(TILE // 8, 8, 128), axis=0)
            return carry

        lax.fori_loop(0, NY, one, 0)

    def add(dx):
        group = GROUP[dx]
        arrive(rl.at[group], rl_recv.at[group])
        acc[group, 1, half[0]] += rl[group, 0]
        acc[group, 3, half[1]] += rl[group, 1]
        for d, tile, side, part in ((1, 1, 0, 0), (-1, 3, 1, 1)):
            src, dst = acc.at[group, tile, half[part]], rs.at[group, side, half[part]]
            go(src, dst, rs_send, rs_recv.at[group], device(dy=d))

    outs = []

    def put(src, dst, n):
        copy = pltpu.make_async_copy(src, dst, out_sem.at[n])
        copy.start()
        outs.append(copy)

    def store(dx):
        group, xx = GROUP[dx], block(dx, 0)[0]
        arrive(rs.at[group], rs_recv.at[group])
        value = acc[group, 0] + rs[group, 0] + rs[group, 1]
        value = value * wa[0, xx].astype(jnp.float32)
        cols = pl.ds(pl.multiple_of(xx * 128, 128), 128)
        masked[group] = value.astype(jnp.bfloat16)
        put(masked.at[group], out_ref.at[:, cols], group)

    def bits_stage(stage):
        if stage == 0:
            for to in XY:
                ref = ixy.at[x * NY + y]
                go(ref, ref, info_send.at[0], info_recv.at[0], device(**to))
            return
        if stage == 1:
            arrive(ixy.at[pl.ds(0, len(XY))], info_recv.at[0])
            rows = pl.ds((z * 2 + c) * NX, NX)
            for k in range(NX):
                line = [ixy[k * NY + n] for n in range(NY)]
                info[(z * 2 + c) * NX + k] = line[0] + line[1] + line[2] + line[3]
            for to in ZC:
                go(info.at[rows], info.at[rows], info_send.at[1], info_recv.at[1], device(**to))
            return
        arrive(info.at[pl.ds(0, NX * len(ZC))], info_recv.at[1])
        line = lax.broadcasted_iota(jnp.int32, (64, 128), 0)
        lanes = lax.broadcasted_iota(jnp.int32, (64, 128), 1)
        table = jnp.zeros((64, 128), jnp.float32)
        for i in range(64):
            xi, zi, ci = i // 16, (i // 2) % 8, i % 2
            table = jnp.where(line == i, info[(zi * 2 + ci) * NX + xi], table)
        tail = lanes >= 64
        bp = jnp.where(tail & (table > 1.5), 1.0, 0.0)
        wp = jnp.where(tail, table - 2.0 * bp, 0.0)
        ap = jnp.where(tail, 0.0, table).astype(jnp.bfloat16)
        wide = jnp.concatenate([bp, jnp.zeros_like(bp)], axis=0).astype(jnp.bfloat16)
        link = jnp.dot(ap, wide, preferred_element_type=jnp.float32)
        present = jnp.where(link > 0.5, wp, 0.0)
        left = (
            lax.broadcasted_iota(jnp.int32, (128, 128), 0)
            < lax.broadcasted_iota(jnp.int32, (128, 128), 1)
        )
        marks = present.astype(jnp.bfloat16)
        inside = jnp.dot(marks, jnp.where(left, 1.0, 0.0).astype(jnp.bfloat16),
                         preferred_element_type=jnp.float32)
        own = line == row
        earlier = jnp.sum(jnp.where(line < row, present, 0.0))
        before = jnp.sum(jnp.where(own, inside, 0.0), axis=0, keepdims=True) + earlier
        here = jnp.sum(jnp.where(own, present, 0.0), axis=0, keepdims=True)
        slots = jnp.where(here > 0.5, before, -1.0)
        for t in range(2):
            here = jnp.where(lane == 64 + 2 * y + t, slots, 0.0)
            slots_v[:, pl.ds(t, 1)] = jnp.sum(here, axis=1, keepdims=True)
        put(slots_v, slot_ref, 4)

    def sum_stage(k):
        if k == 0:
            value = jnp.sum(tot[...], axis=0, keepdims=True)
            first, size, mine, peers = 0, 16, z * 2 + c, ZC
        else:
            arrive(ta.at[pl.ds(16 * (k - 1), 15)], sum_recv.at[k - 1])
            value = ta[16 * (k - 1)]
            for n in range(1, 16):
                value = value + ta[16 * (k - 1) + n]
            first, size, mine, peers = 16, 16, x * NY + y, XY
        if k == 2:
            total_ref[0, 0] = jnp.sum(value) / (TILE * math.sqrt(64 * 8))
            return
        ta[first + mine] = value
        for to in peers:
            ref = ta.at[first + mine]
            go(ref, ref, sum_send, sum_recv.at[k], device(**to))

    run = {
        "step": step, "share": share, "prepare": prepare, "multiply": multiply,
        "weights": weights, "scatter": scatter, "add": add, "store": store,
        "bits": bits_stage, "sum": sum_stage,
    }
    for kind, what in program():
        run[kind](what)
    gone(bg.at[pl.ds(0, (2 * MOVED + 1) * 1024)], bulk_send)
    gone(acc.at[pl.ds(0, 3)], rs_send)
    gone(wa.at[pl.ds(0, 3)], w_send)
    gone(ixy.at[pl.ds(0, 15)], info_send.at[0])
    gone(info.at[pl.ds(0, 60)], info_send.at[1])
    gone(ta.at[pl.ds(0, 30)], sum_send)
    for copy in outs:
        copy.wait()
    for d in (1, 2, 3):
        move(d).wait_send()

    @pl.when(jnp.logical_not(diagonal))
    def _():
        move(0).wait_send()


def hand_over(masked_ref, slot_ref, masked_out, slot_out, masked, slot, sem):
    steps = ((masked_ref, masked, masked_out), (slot_ref, slot, slot_out))
    ins = [pltpu.make_async_copy(a, b, sem.at[n]) for n, (a, b, _) in enumerate(steps)]
    outs = [pltpu.make_async_copy(b, c, sem.at[2 + n]) for n, (_, b, c) in enumerate(steps)]
    for copy in ins:
        copy.start()
    for came, copy in zip(ins, outs):
        came.wait()
        copy.start()
    for copy in outs:
        copy.wait()


def on_device(a_values, a_present, b_values, b_present, w_values, w_present):
    hbm = pl.BlockSpec(memory_space=pltpu.HBM)
    smem = pl.BlockSpec(memory_space=pltpu.SMEM)
    dma = pltpu.SemaphoreType.DMA
    bf16, f32, i32 = jnp.bfloat16, jnp.float32, jnp.int32
    masked, slot, total = pl.pallas_call(
        kernel,
        out_shape=(
            jax.ShapeDtypeStruct((TILE, 512), bf16),
            jax.ShapeDtypeStruct((1, 2), f32),
            jax.ShapeDtypeStruct((1, 1), f32),
        ),
        in_specs=[hbm] * 6,
        out_specs=(hbm, hbm, smem),
        scratch_shapes=[
            pltpu.VMEM((NX * NZ * 2 * 1024, 128), bf16),
            pltpu.VMEM((NZ, TILE, 2 * TILE), bf16),
            pltpu.VMEM((NX, NY, TILE, 128), f32),
            pltpu.VMEM((NX, 2, 128, 128), f32),
            pltpu.VMEM((NX, 2, TILE, 128), f32),
            pltpu.VMEM((NY, NX, TILE, 128), bf16),
            pltpu.VMEM((NX, TILE, 128), bf16),
            pltpu.VMEM((TILE, 512), bf16),
            pltpu.VMEM((TILE, 512), bf16),
            pltpu.VMEM((NX, TILE, 128), bf16),
            pltpu.VMEM((1, 2), f32),
            pltpu.VMEM((8, 128), f32),
            pltpu.VMEM((NX * NY, 1, 128), f32),
            pltpu.VMEM((64, 1, 128), f32),
            pltpu.VMEM((32, 1, 128), f32),
            pltpu.SMEM((1, 16), i32),
            pltpu.SMEM((1, 2), i32),
            pltpu.SMEM((1, 2), i32),
            dma, dma((5,)), dma((5,)), dma((NX,)), dma((NY,)),
            dma, dma((len(KEY_ID),)), dma((len(BLOCKS),)),
            dma, dma, dma, dma((NX,)), dma((NX,)),
            dma((2,)), dma((2,)), dma, dma((2,)),
        ],
        compiler_params=pltpu.CompilerParams(
            collective_id=0, has_side_effects=True, vmem_limit_bytes=60 * 2**20
        ),
    )(a_values, a_present, b_values, b_present, w_values, w_present)
    masked, slot = pl.pallas_call(
        hand_over,
        out_shape=(
            jax.ShapeDtypeStruct((TILE, 512), bf16),
            jax.ShapeDtypeStruct((1, 2), f32),
        ),
        in_specs=[hbm] * 2,
        out_specs=(hbm, hbm),
        scratch_shapes=[
            pltpu.VMEM((TILE, 512), bf16), pltpu.VMEM((1, 2), f32), dma((4,)),
        ],
        compiler_params=pltpu.CompilerParams(vmem_limit_bytes=60 * 2**20),
    )(masked, slot)
    return masked, slot, total.reshape(())


def solution(mesh):
    spec = P("row", "col")
    return jax.shard_map(
        on_device, mesh=mesh, in_specs=(spec,) * 6, out_specs=(spec, spec, P()),
        check_vma=False,
    )
```

```python
import heapq
import math

import jax
import jax.numpy as jnp
from jax import lax
from jax.experimental import pallas as pl
from jax.experimental.pallas import tpu as pltpu
from jax.sharding import PartitionSpec as P

MESH = pl.DeviceIdType.MESH
TILE = 256
NX, NZ, NY = 4, 8, 4
LINKS = ("x+", "x-", "z+", "z-")
PIECES = (
    ("Z", 0, 256, (0,)),
    ("Z", 256, 352, (1, 2)),
    ("X", 608, 416, (2, 3)),
    ("J", 0, 608, ()),
)
JOINED = len(PIECES) - 1
BLOCKS = [(dx, dz) for dx in (0, -1, 1, 2) for dz in (0, -1, 1, -2, 2, -3, 3, 4)]
BLOCK_ID = {block: n for n, block in enumerate(BLOCKS)}
GROUP = {0: 0, -1: 1, 1: 2, 2: 3}
KEYS = [
    (p, *block)
    for p in range(len(PIECES))
    for block in BLOCKS[1:]
    if {"Z": block[0] == 0, "X": True, "J": block[0] != 0}[PIECES[p][0]]
]
KEY_ID = {key: n for n, key in enumerate(KEYS)}
MOVED = NX * NZ - 1
LATENCY, Y_LATENCY, RATE, LEAD = 2.5, 3.0, 46.6e3, 1.85
STEP, MULTIPLY, SHARE = 0.03, 0.47, 1.5
READY = (0.0, 0.8, 1.2)
BITS = (1.0, 12.0, 30.0)
SUM = 3.8


def rank_z(p, dx, dz):
    return -1.0 if PIECES[p][0] == "Z" else abs(dx) - 0.6 * abs(dz)


def rank_x(p, dx):
    return {"X": (-1.0, 0.0), "J": (1.0, 2.0)}[PIECES[p][0]][abs(dx)]


def program():
    free = dict.fromkeys(LINKS + ("y+", "y-"), 0.0)
    waiting = {link: [] for link in LINKS}
    inbox, ready, items, count = [], [], [], [0]
    missing = {block: 2 if block[0] else len(PIECES) - 1 for block in BLOCKS}
    unjoined = {dz: 2 for dx, dz in BLOCKS if dx == 0}
    left = {dx: NZ for dx in GROUP}

    def push(heap, when, what):
        count[0] += 1
        heapq.heappush(heap, (when, count[0], what))

    def commit(now):
        sends = []
        for link in LINKS:
            while waiting[link] and free[link] - now < LEAD:
                key = heapq.heappop(waiting[link])[2]
                free[link] = max(now, free[link]) + PIECES[key[0]][2] * 256 / RATE
                push(inbox, free[link] + LATENCY, key)
                sends.append((link, key))
        return tuple(sends)

    def along_y(link, now, rows):
        free[link] = max(now, free[link]) + rows * 512 / RATE
        return free[link] + Y_LATENCY

    def along_z(p, dx, dz):
        rank = rank_z(p, dx, dz)
        if dz == 0:
            push(waiting["z+"], rank, (p, dx, -1))
            push(waiting["z-"], rank, (p, dx, 1))
        elif abs(dz) < 3:
            sign = 1 if dz > 0 else -1
            push(waiting["z-" if dz > 0 else "z+"], rank, (p, dx, dz + sign))
        elif abs(dz) == 3:
            sign = -1 if (p + abs(dx) // 2 + (dx == 1)) % 2 == 0 else 1
            if (dz < 0) == (sign < 0):
                push(waiting["z-" if dz > 0 else "z+"], rank, (p, dx, 4))

    def along_x(p, dx, dz):
        rank = rank_x(p, dx) if abs(dx) < 2 else 0.0
        if dx == 0:
            push(waiting["x+"], rank, (p, -1, dz))
            push(waiting["x-"], rank, (p, 1, dz))
        elif dx == (-1 if (p + dz) % 2 == 0 else 1):
            push(waiting["x+" if dx < 0 else "x-"], rank, (p, 2, dz))

    for p, when in enumerate(READY):
        push(inbox, when, (p, 0, 0))
    for stage, when in enumerate(BITS):
        push(ready, when, ("bits", stage))
    push(ready, 3.0, ("weights", None))
    push(ready, 2.5, ("prepare", None))
    now = 0.0
    while inbox or ready:
        if inbox and inbox[0][0] <= now:
            key = heapq.heappop(inbox)[2]
            p, dx, dz = key
            if PIECES[p][0] == "Z":
                along_z(*key)
                unjoined[dz] -= 1
                if unjoined[dz] == 0:
                    along_x(JOINED, 0, dz)
            elif PIECES[p][0] == "J":
                along_x(*key)
            else:
                if dz == 0:
                    along_x(*key)
                along_z(*key)
            now += STEP
            sends = commit(now)
            items.append(("step", (key, sends)))
            block = dx, dz
            missing[block] -= 1
            if missing[block] == 0:
                items.append(("share", block))
                push(ready, now + SHARE, ("multiply", block))
        elif ready and ready[0][0] <= now:
            kind, what = heapq.heappop(ready)[2]
            items.append((kind, what))
            if kind == "multiply":
                now += MULTIPLY
                dx = what[0]
                left[dx] -= 1
                if left[dx] == 0:
                    items.append(("scatter", dx))
                    now += 0.25
                    first = max(along_y("y+", now, 128), along_y("y-", now, 128))
                    along_y("y+", now, 128), along_y("y-", now, 128)
                    push(ready, first, ("add", dx))
                    if not any(left.values()):
                        push(ready, now, ("sum", 0))
            elif kind == "add":
                now += 0.15
                last = max(along_y("y+", now, 128), along_y("y-", now, 128))
                push(ready, last, ("store", what))
            elif kind == "sum" and what < 2:
                push(ready, now + SUM, ("sum", what + 1))
            elif kind == "prepare":
                now += 0.3
            elif kind == "store":
                now += 0.1
            sends = commit(now)
            if sends:
                items.append(("step", (None, sends)))
        else:
            now = min(heap[0][0] for heap in (inbox, ready) if heap)
    return items


def kernel(
    a_ref, ap_ref, b_ref, bp_ref, w_ref, wp_ref,
    out_ref, slot_ref, total_ref,
    bg, ae, acc, rl, rs, wa, bm, braw, wraw, tot, ixy, info, ta, ap, bp, wp,
    a_sem, in_sem, move_send, move_recv, bulk_send, piece_recv, share_recv,
    w_send, w_recv, rs_send, rl_recv, rs_recv, info_send, info_recv, sum_send, sum_recv,
):
    row, y = lax.axis_index("row"), lax.axis_index("col")
    c = lax.rem(row, 2)
    z = lax.rem(row // 2, NZ)
    x = row // (2 * NZ)

    def device(dx=0, dy=0, dz=0, dc=0):
        xx, zz = lax.rem(x + dx + NX, NX), lax.rem(z + dz + NZ, NZ)
        return ((xx * NZ + zz) * 2 + lax.rem(c + dc, 2), lax.rem(y + dy + NY, NY))

    def place(xx, yy):
        return ((xx * NZ + z) * 2 + c, yy)

    def remote(src, dst, send, recv, to):
        return pltpu.make_async_remote_copy(
            src_ref=src, dst_ref=dst, send_sem=send, recv_sem=recv,
            device_id=to, device_id_type=MESH,
        )

    def arrive(dst, recv):
        remote(dst, dst, sum_send, recv, device(dc=1)).wait_recv()

    def gone(src, send):
        remote(src, src, send, sum_recv.at[0], device(dc=1)).wait_send()

    def go(*args):
        remote(*args).start()

    def at(xx, zz, core, first=0, size=1024):
        start = ((xx * NZ + zz) * 2 + core) * 1024 + first
        return pl.ds(pl.multiple_of(start, 16), size)

    ZC = [{"dz": d, "dc": e} for d in range(NZ) for e in range(2)][1:]
    XY = [{"dx": d, "dy": e} for d in range(NX) for e in range(NY)][1:]

    loads = [
        pltpu.make_async_copy(src, dst, in_sem.at[n])
        for n, (src, dst) in enumerate(
            ((b_ref, braw), (bp_ref, bp), (ap_ref, ap), (wp_ref, wp), (w_ref, wraw))
        )
    ]
    for k in range(NZ):
        loads.append(pltpu.make_async_copy(
            a_ref.at[:, pl.ds(k * 2 * TILE, 2 * TILE)], ae.at[k], a_sem
        ))
    for load in loads:
        load.start()
    barrier = pltpu.get_barrier_semaphore()

    def greet(to):
        pl.semaphore_signal(barrier, inc=1, device_id=to, device_id_type=MESH)

    for to in ZC + XY:
        greet(device(**to))

    def flag(ref, n):
        return ref[0, n].astype(jnp.float32).astype(jnp.bfloat16)

    for load in loads[:2]:
        load.wait()
    for q in range(NX):
        bm[q] = braw[:, pl.ds(q * 128, 128)] * flag(bp, q // 2)
    for load in loads[2:4]:
        load.wait()
    lane = lax.broadcasted_iota(jnp.int32, (1, 128), 1)
    bits = jnp.zeros((1, 128), jnp.float32)
    for t in range(16):
        bits = jnp.where(lane == 16 * y + t, ap[0, t].astype(jnp.float32), bits)
    for t in range(2):
        both = wp[0, t] + 2 * bp[0, t]
        bits = jnp.where(lane == 64 + 2 * y + t, both.astype(jnp.float32), bits)
    ixy[x * NY + y] = bits
    pl.semaphore_wait(barrier, len(ZC + XY))

    diagonal = x == y
    mine = lax.rem(y - x + NY, NY)

    def move(d):
        q = lax.rem(x + d, NX)
        dst = bg.at[at(q, z, c, mine * TILE, TILE)]
        return remote(bm.at[q], dst, move_send.at[d], move_recv.at[mine], place(q, x))

    for d in (2, 1, 3):
        move(d).start()

    @pl.when(jnp.logical_not(diagonal))
    def _():
        move(0).start()

    @pl.when(diagonal)
    def _():
        bg[at(x, z, c, mine * TILE, TILE)] = bm[x]

    landed = set()

    def land(j):
        if j in landed:
            return
        landed.add(j)
        dst = bg.at[at(x, z, c, j * TILE, TILE)]
        if j > 0:
            arrive(dst, move_recv.at[j])
            return

        @pl.when(jnp.logical_not(diagonal))
        def _():
            arrive(dst, move_recv.at[0])

    def block(dx, dz):
        return lax.rem(x + dx + NX, NX), lax.rem(z + dz + NZ, NZ)

    def piece(key, dx=0, dz=0):
        _, first, size, _ = PIECES[key[0]]
        xx, zz = block(key[1] + dx, key[2] + dz)
        return bg.at[at(xx, zz, c, first, size)]

    def step(what):
        key, sends = what
        if key is not None:
            if key[1:] == (0, 0):
                for tile in PIECES[key[0]][3]:
                    land(tile)
            else:
                arrive(piece(key), piece_recv.at[KEY_ID[key]])
        for link, out in sends:
            d = 1 if link[1] == "+" else -1
            to = {"dx": d} if link[0] == "x" else {"dz": d}
            ref, n = piece(out, **to), KEY_ID[out]
            go(ref, ref, bulk_send, piece_recv.at[n], device(**to))

    def share(what):
        n, (xx, zz) = BLOCK_ID[what], block(*what)
        ref = bg.at[at(xx, zz, c)]
        go(ref, ref, bulk_send, share_recv.at[n], device(dc=1))

    def prepare(_):
        loads[4].wait()
        pltpu.make_async_copy(ae, ae, a_sem).wait()
        for q in range(NX):
            wa[0, q] = wraw[:, pl.ds(q * 128, 128)] * flag(wp, q // 2)
        for k in range(NZ):
            for t in range(2):
                cols = pl.ds(t * TILE, TILE)
                ae[k, :, cols] = ae[k, :, cols] * flag(ap, 2 * k + t)

    begun = set()

    def multiply(what):
        n, (xx, zz) = BLOCK_ID[what], block(*what)
        arrive(bg.at[at(xx, zz, 1 - c)], share_recv.at[n])
        group = GROUP[what[0]]
        fresh = group not in begun
        begun.add(group)

        for p in range(2):

            def part(core, t):
                return bg[at(xx, zz, core, (2 * p + t) * TILE, TILE), :]

            right = jnp.concatenate(
                [jnp.concatenate([part(k, 0), part(k, 1)], axis=1) for k in range(2)], axis=0
            )
            new = jnp.dot(ae[zz], right, preferred_element_type=jnp.float32)
            for t in range(2):
                new_t = new[:, t * 128 : (t + 1) * 128]
                acc[group, 2 * p + t] = new_t if fresh else acc[group, 2 * p + t] + new_t

    def weights(_):
        for d in range(1, NY):
            go(wa.at[0], wa.at[NY - d], w_send, w_recv, device(dy=d))

    heard = []
    half = (pl.ds(0, 128), pl.ds(128, 128))

    def scatter(dx):
        group, xx = GROUP[dx], block(dx, 0)[0]
        for d, src, dst, recv in (
            (1, acc.at[group, 2, half[0]], rl.at[group, 0], rl_recv),
            (-1, acc.at[group, 2, half[1]], rl.at[group, 1], rl_recv),
            (1, acc.at[group, 1, half[1]], rs.at[group, 0, half[1]], rs_recv),
            (-1, acc.at[group, 3, half[0]], rs.at[group, 1, half[0]], rs_recv),
        ):
            go(src, dst, rs_send, recv.at[group], device(dy=d))
        if not heard:
            heard.append(True)
            tot[...] = jnp.zeros_like(tot)
            arrive(wa.at[pl.ds(1, NY - 1)], w_recv)

        def one(j, carry):
            value = acc[group, j] * wa[j, xx].astype(jnp.float32)
            tot[...] += jnp.sum(value.reshape(TILE // 8, 8, 128), axis=0)
            return carry

        lax.fori_loop(0, NY, one, 0)

    def add(dx):
        group = GROUP[dx]
        arrive(rl.at[group], rl_recv.at[group])
        acc[group, 1, half[0]] += rl[group, 0]
        acc[group, 3, half[1]] += rl[group, 1]
        for d, tile, side, part in ((1, 1, 0, 0), (-1, 3, 1, 1)):
            src, dst = acc.at[group, tile, half[part]], rs.at[group, side, half[part]]
            go(src, dst, rs_send, rs_recv.at[group], device(dy=d))

    def store(dx):
        group, xx = GROUP[dx], block(dx, 0)[0]
        arrive(rs.at[group], rs_recv.at[group])
        value = acc[group, 0] + rs[group, 0] + rs[group, 1]
        value = value * wa[0, xx].astype(jnp.float32)
        cols = pl.ds(pl.multiple_of(xx * 128, 128), 128)
        out_ref[:, cols] = value.astype(jnp.bfloat16)

    def bits_stage(stage):
        if stage == 0:
            for to in XY:
                ref = ixy.at[x * NY + y]
                go(ref, ref, info_send.at[0], info_recv.at[0], device(**to))
            return
        if stage == 1:
            arrive(ixy.at[pl.ds(0, len(XY))], info_recv.at[0])
            rows = pl.ds((z * 2 + c) * NX, NX)
            for k in range(NX):
                line = [ixy[k * NY + n] for n in range(NY)]
                info[(z * 2 + c) * NX + k] = line[0] + line[1] + line[2] + line[3]
            for to in ZC:
                go(info.at[rows], info.at[rows], info_send.at[1], info_recv.at[1], device(**to))
            return
        arrive(info.at[pl.ds(0, NX * len(ZC))], info_recv.at[1])
        line = lax.broadcasted_iota(jnp.int32, (64, 128), 0)
        lanes = lax.broadcasted_iota(jnp.int32, (64, 128), 1)
        table = jnp.zeros((64, 128), jnp.float32)
        for i in range(64):
            xi, zi, ci = i // 16, (i // 2) % 8, i % 2
            table = jnp.where(line == i, info[(zi * 2 + ci) * NX + xi], table)
        tail = lanes >= 64
        bp = jnp.where(tail & (table > 1.5), 1.0, 0.0)
        wp = jnp.where(tail, table - 2.0 * bp, 0.0)
        ap = jnp.where(tail, 0.0, table).astype(jnp.bfloat16)
        wide = jnp.concatenate([bp, jnp.zeros_like(bp)], axis=0).astype(jnp.bfloat16)
        link = jnp.dot(ap, wide, preferred_element_type=jnp.float32)
        present = jnp.where(link > 0.5, wp, 0.0)
        left = (
            lax.broadcasted_iota(jnp.int32, (128, 128), 0)
            < lax.broadcasted_iota(jnp.int32, (128, 128), 1)
        )
        marks = present.astype(jnp.bfloat16)
        inside = jnp.dot(marks, jnp.where(left, 1.0, 0.0).astype(jnp.bfloat16),
                         preferred_element_type=jnp.float32)
        own = line == row
        earlier = jnp.sum(jnp.where(line < row, present, 0.0))
        before = jnp.sum(jnp.where(own, inside, 0.0), axis=0, keepdims=True) + earlier
        here = jnp.sum(jnp.where(own, present, 0.0), axis=0, keepdims=True)
        slots = jnp.where(here > 0.5, before, -1.0)
        for t in range(2):
            here = jnp.where(lane == 64 + 2 * y + t, slots, 0.0)
            slot_ref[:, pl.ds(t, 1)] = jnp.sum(here, axis=1, keepdims=True)

    def sum_stage(k):
        if k == 0:
            value = jnp.sum(tot[...], axis=0, keepdims=True)
            first, size, mine, peers = 0, 16, z * 2 + c, ZC
        else:
            arrive(ta.at[pl.ds(16 * (k - 1), 15)], sum_recv.at[k - 1])
            value = ta[16 * (k - 1)]
            for n in range(1, 16):
                value = value + ta[16 * (k - 1) + n]
            first, size, mine, peers = 16, 16, x * NY + y, XY
        if k == 2:
            total_ref[0, 0] = jnp.sum(value) / (TILE * math.sqrt(64 * 8))
            return
        ta[first + mine] = value
        for to in peers:
            ref = ta.at[first + mine]
            go(ref, ref, sum_send, sum_recv.at[k], device(**to))

    run = {
        "step": step, "share": share, "prepare": prepare, "multiply": multiply,
        "weights": weights, "scatter": scatter, "add": add, "store": store,
        "bits": bits_stage, "sum": sum_stage,
    }
    for kind, what in program():
        run[kind](what)
    gone(bg.at[pl.ds(0, (2 * MOVED + 1) * 1024)], bulk_send)
    gone(acc.at[pl.ds(0, 3)], rs_send)
    gone(wa.at[pl.ds(0, 3)], w_send)
    gone(ixy.at[pl.ds(0, 15)], info_send.at[0])
    gone(info.at[pl.ds(0, 60)], info_send.at[1])
    gone(ta.at[pl.ds(0, 30)], sum_send)
    for d in (1, 2, 3):
        move(d).wait_send()

    @pl.when(jnp.logical_not(diagonal))
    def _():
        move(0).wait_send()


def hand_over(masked, slot, masked_out, slot_out, sem):
    copies = [
        pltpu.make_async_copy(src, dst, sem.at[n])
        for n, (src, dst) in enumerate(((masked, masked_out), (slot, slot_out)))
    ]
    for copy in copies:
        copy.start()
    for copy in copies:
        copy.wait()


def on_device(a_values, a_present, b_values, b_present, w_values, w_present):
    hbm = pl.BlockSpec(memory_space=pltpu.HBM)
    smem = pl.BlockSpec(memory_space=pltpu.SMEM)
    vmem = pl.BlockSpec(memory_space=pltpu.VMEM)
    dma = pltpu.SemaphoreType.DMA
    bf16, f32, i32 = jnp.bfloat16, jnp.float32, jnp.int32
    masked, slot, total = pl.pallas_call(
        kernel,
        out_shape=(
            jax.ShapeDtypeStruct((TILE, 512), bf16),
            jax.ShapeDtypeStruct((1, 2), f32),
            jax.ShapeDtypeStruct((1, 1), f32),
        ),
        in_specs=[hbm] * 6,
        out_specs=(vmem, vmem, smem),
        scratch_shapes=[
            pltpu.VMEM((NX * NZ * 2 * 1024, 128), bf16),
            pltpu.VMEM((NZ, TILE, 2 * TILE), bf16),
            pltpu.VMEM((NX, NY, TILE, 128), f32),
            pltpu.VMEM((NX, 2, 128, 128), f32),
            pltpu.VMEM((NX, 2, TILE, 128), f32),
            pltpu.VMEM((NY, NX, TILE, 128), bf16),
            pltpu.VMEM((NX, TILE, 128), bf16),
            pltpu.VMEM((TILE, 512), bf16),
            pltpu.VMEM((TILE, 512), bf16),
            pltpu.VMEM((8, 128), f32),
            pltpu.VMEM((NX * NY, 1, 128), f32),
            pltpu.VMEM((64, 1, 128), f32),
            pltpu.VMEM((32, 1, 128), f32),
            pltpu.SMEM((1, 16), i32),
            pltpu.SMEM((1, 2), i32),
            pltpu.SMEM((1, 2), i32),
            dma, dma((5,)), dma((NX,)), dma((NY,)),
            dma, dma((len(KEY_ID),)), dma((len(BLOCKS),)),
            dma, dma, dma, dma((NX,)), dma((NX,)),
            dma((2,)), dma((2,)), dma, dma((2,)),
        ],
        compiler_params=pltpu.CompilerParams(
            collective_id=0, has_side_effects=True, vmem_limit_bytes=48 * 2**20
        ),
    )(*[
        pltpu.with_memory_space_constraint(v, pltpu.HBM)
        for v in (a_values, a_present, b_values, b_present, w_values, w_present)
    ])
    masked, slot = pl.pallas_call(
        hand_over,
        out_shape=(
            jax.ShapeDtypeStruct((TILE, 512), bf16),
            jax.ShapeDtypeStruct((1, 2), f32),
        ),
        in_specs=[vmem] * 2,
        out_specs=(hbm, hbm),
        scratch_shapes=[dma((2,))],
        compiler_params=pltpu.CompilerParams(vmem_limit_bytes=2**20),
    )(masked, slot)
    return masked, slot, total.reshape(())


def solution(mesh):
    spec = P("row", "col")
    return jax.shard_map(
        on_device, mesh=mesh, in_specs=(spec,) * 6, out_specs=(spec, spec, P()),
        check_vma=False,
    )
```

```python
import heapq
import math

import jax
import jax.numpy as jnp
from jax import lax
from jax.experimental import pallas as pl
from jax.experimental.pallas import tpu as pltpu
from jax.sharding import PartitionSpec as P

MESH = pl.DeviceIdType.MESH
TILE = 256
NX, NZ, NY = 4, 8, 4
LINKS = ("x+", "x-", "z+", "z-")
PIECES = (
    ("Z", 0, 256, (0,)),
    ("Z", 256, 352, (1, 2)),
    ("X", 608, 416, (2, 3)),
    ("J", 0, 608, ()),
)
JOINED = len(PIECES) - 1
BLOCKS = [(dx, dz) for dx in (0, -1, 1, 2) for dz in (0, -1, 1, -2, 2, -3, 3, 4)]
BLOCK_ID = {block: n for n, block in enumerate(BLOCKS)}
GROUP = {0: 0, -1: 1, 1: 2, 2: 3}
KEYS = [
    (p, *block)
    for p in range(len(PIECES))
    for block in BLOCKS[1:]
    if {"Z": block[0] == 0, "X": True, "J": block[0] != 0}[PIECES[p][0]]
]
KEY_ID = {key: n for n, key in enumerate(KEYS)}
MOVED = NX * NZ - 1
LATENCY, Y_LATENCY, RATE, LEAD = 2.5, 3.0, 46.6e3, 1.85
STEP, MULTIPLY, SHARE = 0.03, 0.47, 1.5
READY = (0.0, 0.8, 1.2)
BITS = (1.0, 12.0, 30.0)
SUM = 3.8


def rank_z(p, dx, dz):
    return -1.0 if PIECES[p][0] == "Z" else abs(dx) - 0.6 * abs(dz)


def rank_x(p, dx):
    return {"X": (-1.0, 0.0), "J": (1.0, 2.0)}[PIECES[p][0]][abs(dx)]


def program():
    free = dict.fromkeys(LINKS + ("y+", "y-"), 0.0)
    waiting = {link: [] for link in LINKS}
    inbox, ready, items, count = [], [], [], [0]
    missing = {block: 2 if block[0] else len(PIECES) - 1 for block in BLOCKS}
    unjoined = {dz: 2 for dx, dz in BLOCKS if dx == 0}
    left = {dx: NZ for dx in GROUP}

    def push(heap, when, what):
        count[0] += 1
        heapq.heappush(heap, (when, count[0], what))

    def commit(now):
        sends = []
        for link in LINKS:
            while waiting[link] and free[link] - now < LEAD:
                key = heapq.heappop(waiting[link])[2]
                free[link] = max(now, free[link]) + PIECES[key[0]][2] * 256 / RATE
                push(inbox, free[link] + LATENCY, key)
                sends.append((link, key))
        return tuple(sends)

    def along_y(link, now, rows):
        free[link] = max(now, free[link]) + rows * 512 / RATE
        return free[link] + Y_LATENCY

    def along_z(p, dx, dz):
        rank = rank_z(p, dx, dz)
        if dz == 0:
            push(waiting["z+"], rank, (p, dx, -1))
            push(waiting["z-"], rank, (p, dx, 1))
        elif abs(dz) < 3:
            sign = 1 if dz > 0 else -1
            push(waiting["z-" if dz > 0 else "z+"], rank, (p, dx, dz + sign))
        elif abs(dz) == 3:
            sign = -1 if (p + abs(dx) // 2 + (dx == 1)) % 2 == 0 else 1
            if (dz < 0) == (sign < 0):
                push(waiting["z-" if dz > 0 else "z+"], rank, (p, dx, 4))

    def along_x(p, dx, dz):
        rank = rank_x(p, dx) if abs(dx) < 2 else 0.0
        if dx == 0:
            push(waiting["x+"], rank, (p, -1, dz))
            push(waiting["x-"], rank, (p, 1, dz))
        elif dx == (-1 if (p + dz) % 2 == 0 else 1):
            push(waiting["x+" if dx < 0 else "x-"], rank, (p, 2, dz))

    for p, when in enumerate(READY):
        push(inbox, when, (p, 0, 0))
    for stage, when in enumerate(BITS):
        push(ready, when, ("bits", stage))
    push(ready, 3.0, ("weights", None))
    push(ready, 2.5, ("prepare", None))
    now = 0.0
    while inbox or ready:
        if inbox and inbox[0][0] <= now:
            key = heapq.heappop(inbox)[2]
            p, dx, dz = key
            if PIECES[p][0] == "Z":
                along_z(*key)
                unjoined[dz] -= 1
                if unjoined[dz] == 0:
                    along_x(JOINED, 0, dz)
            elif PIECES[p][0] == "J":
                along_x(*key)
            else:
                if dz == 0:
                    along_x(*key)
                along_z(*key)
            now += STEP
            sends = commit(now)
            items.append(("step", (key, sends)))
            block = dx, dz
            missing[block] -= 1
            if missing[block] == 0:
                push(ready, now + SHARE, ("multiply", block))
        elif ready and ready[0][0] <= now:
            kind, what = heapq.heappop(ready)[2]
            items.append((kind, what))
            if kind == "multiply":
                now += MULTIPLY
                dx = what[0]
                left[dx] -= 1
                if left[dx] == 0:
                    items.append(("scatter", dx))
                    now += 0.25
                    first = max(along_y("y+", now, 128), along_y("y-", now, 128))
                    along_y("y+", now, 128), along_y("y-", now, 128)
                    push(ready, first, ("add", dx))
                    if not any(left.values()):
                        push(ready, now, ("sum", 0))
            elif kind == "add":
                now += 0.15
                last = max(along_y("y+", now, 128), along_y("y-", now, 128))
                push(ready, last, ("store", what))
            elif kind == "sum" and what < 2:
                push(ready, now + SUM, ("sum", what + 1))
            elif kind == "prepare":
                now += 0.3
            elif kind == "store":
                now += 0.1
            sends = commit(now)
            if sends:
                items.append(("step", (None, sends)))
        else:
            now = min(heap[0][0] for heap in (inbox, ready) if heap)
    return items


def kernel(
    a_ref, ap_ref, b_ref, bp_ref, w_ref, wp_ref,
    out_ref, slot_ref, total_ref,
    bg, ae, acc, rl, rs, wa, bm, braw, wraw, tot, ixy, info, ta, ap, bp, wp,
    a_sem, in_sem, move_send, move_recv, bulk_send, piece_recv, share_recv,
    w_send, w_recv, rs_send, rl_recv, rs_recv, info_send, info_recv, sum_send, sum_recv,
):
    row, y = lax.axis_index("row"), lax.axis_index("col")
    c = lax.rem(row, 2)
    z = lax.rem(row // 2, NZ)
    x = row // (2 * NZ)

    def device(dx=0, dy=0, dz=0, dc=0):
        xx, zz = lax.rem(x + dx + NX, NX), lax.rem(z + dz + NZ, NZ)
        return ((xx * NZ + zz) * 2 + lax.rem(c + dc, 2), lax.rem(y + dy + NY, NY))

    def place(xx, yy):
        return ((xx * NZ + z) * 2 + c, yy)

    def remote(src, dst, send, recv, to):
        return pltpu.make_async_remote_copy(
            src_ref=src, dst_ref=dst, send_sem=send, recv_sem=recv,
            device_id=to, device_id_type=MESH,
        )

    def arrive(dst, recv):
        remote(dst, dst, sum_send, recv, device(dc=1)).wait_recv()

    def gone(src, send):
        remote(src, src, send, sum_recv.at[0], device(dc=1)).wait_send()

    def go(*args):
        remote(*args).start()

    def at(xx, zz, core, first=0, size=1024):
        start = ((xx * NZ + zz) * 2 + core) * 1024 + first
        return pl.ds(pl.multiple_of(start, 16), size)

    ZC = [{"dz": d, "dc": e} for d in range(NZ) for e in range(2)][1:]
    XY = [{"dx": d, "dy": e} for d in range(NX) for e in range(NY)][1:]

    loads = [
        pltpu.make_async_copy(src, dst, in_sem.at[n])
        for n, (src, dst) in enumerate(
            ((b_ref, braw), (bp_ref, bp), (ap_ref, ap), (wp_ref, wp), (w_ref, wraw))
        )
    ]
    for k in range(NZ):
        loads.append(pltpu.make_async_copy(
            a_ref.at[:, pl.ds(k * 2 * TILE, 2 * TILE)], ae.at[k], a_sem
        ))
    for load in loads:
        load.start()
    barrier = pltpu.get_barrier_semaphore()

    def greet(to):
        pl.semaphore_signal(barrier, inc=1, device_id=to, device_id_type=MESH)

    for to in ZC + XY:
        greet(device(**to))

    def flag(ref, n):
        return ref[0, n].astype(jnp.float32).astype(jnp.bfloat16)

    for load in loads[:2]:
        load.wait()
    for q in range(NX):
        bm[q] = braw[:, pl.ds(q * 128, 128)] * flag(bp, q // 2)
    for load in loads[2:4]:
        load.wait()
    lane = lax.broadcasted_iota(jnp.int32, (1, 128), 1)
    bits = jnp.zeros((1, 128), jnp.float32)
    for t in range(16):
        bits = jnp.where(lane == 16 * y + t, ap[0, t].astype(jnp.float32), bits)
    for t in range(2):
        both = wp[0, t] + 2 * bp[0, t]
        bits = jnp.where(lane == 64 + 2 * y + t, both.astype(jnp.float32), bits)
    ixy[x * NY + y] = bits
    pl.semaphore_wait(barrier, len(ZC + XY))

    diagonal = x == y
    mine = lax.rem(y - x + NY, NY)

    def move(d):
        q = lax.rem(x + d, NX)
        dst = bg.at[at(q, z, c, mine * TILE, TILE)]
        return remote(bm.at[q], dst, move_send.at[d], move_recv.at[mine], place(q, x))

    for d in (2, 1, 3):
        move(d).start()

    @pl.when(jnp.logical_not(diagonal))
    def _():
        move(0).start()

    @pl.when(diagonal)
    def _():
        bg[at(x, z, c, mine * TILE, TILE)] = bm[x]

    landed = set()

    def land(j):
        if j in landed:
            return
        landed.add(j)
        dst = bg.at[at(x, z, c, j * TILE, TILE)]
        if j > 0:
            arrive(dst, move_recv.at[j])
            return

        @pl.when(jnp.logical_not(diagonal))
        def _():
            arrive(dst, move_recv.at[0])

    def block(dx, dz):
        return lax.rem(x + dx + NX, NX), lax.rem(z + dz + NZ, NZ)

    def piece(key, dx=0, dz=0):
        _, first, size, _ = PIECES[key[0]]
        xx, zz = block(key[1] + dx, key[2] + dz)
        return bg.at[at(xx, zz, c, first, size)]

    def step(what):
        key, sends = what
        if key is not None:
            if key[1:] == (0, 0):
                for tile in PIECES[key[0]][3]:
                    land(tile)
            else:
                arrive(piece(key), piece_recv.at[KEY_ID[key]])
        for link, out in sends:
            d = 1 if link[1] == "+" else -1
            to = {"dx": d} if link[0] == "x" else {"dz": d}
            ref, n = piece(out, **to), KEY_ID[out]
            go(ref, ref, bulk_send, piece_recv.at[n], device(**to))
        if key is not None:
            ref, n = piece(key), BLOCK_ID[key[1:]]
            go(ref, ref, bulk_send, share_recv.at[n], device(dc=1))

    def prepare(_):
        loads[4].wait()
        pltpu.make_async_copy(ae, ae, a_sem).wait()
        for q in range(NX):
            wa[0, q] = wraw[:, pl.ds(q * 128, 128)] * flag(wp, q // 2)
        for k in range(NZ):
            for t in range(2):
                cols = pl.ds(t * TILE, TILE)
                ae[k, :, cols] = ae[k, :, cols] * flag(ap, 2 * k + t)

    begun = set()

    def multiply(what):
        n, (xx, zz) = BLOCK_ID[what], block(*what)
        arrive(bg.at[at(xx, zz, 1 - c)], share_recv.at[n])
        group = GROUP[what[0]]
        fresh = group not in begun
        begun.add(group)

        for p in range(2):

            def part(core, t):
                return bg[at(xx, zz, core, (2 * p + t) * TILE, TILE), :]

            right = jnp.concatenate(
                [jnp.concatenate([part(k, 0), part(k, 1)], axis=1) for k in range(2)], axis=0
            )
            new = jnp.dot(ae[zz], right, preferred_element_type=jnp.float32)
            for t in range(2):
                new_t = new[:, t * 128 : (t + 1) * 128]
                acc[group, 2 * p + t] = new_t if fresh else acc[group, 2 * p + t] + new_t

    def weights(_):
        for d in range(1, NY):
            go(wa.at[0], wa.at[NY - d], w_send, w_recv, device(dy=d))

    heard = []
    half = (pl.ds(0, 128), pl.ds(128, 128))

    def scatter(dx):
        group, xx = GROUP[dx], block(dx, 0)[0]
        for d, src, dst, recv in (
            (1, acc.at[group, 2, half[0]], rl.at[group, 0], rl_recv),
            (-1, acc.at[group, 2, half[1]], rl.at[group, 1], rl_recv),
            (1, acc.at[group, 1, half[1]], rs.at[group, 0, half[1]], rs_recv),
            (-1, acc.at[group, 3, half[0]], rs.at[group, 1, half[0]], rs_recv),
        ):
            go(src, dst, rs_send, recv.at[group], device(dy=d))
        if not heard:
            heard.append(True)
            tot[...] = jnp.zeros_like(tot)
            arrive(wa.at[pl.ds(1, NY - 1)], w_recv)

        def one(j, carry):
            value = acc[group, j] * wa[j, xx].astype(jnp.float32)
            tot[...] += jnp.sum(value.reshape(TILE // 8, 8, 128), axis=0)
            return carry

        lax.fori_loop(0, NY, one, 0)

    def add(dx):
        group = GROUP[dx]
        arrive(rl.at[group], rl_recv.at[group])
        acc[group, 1, half[0]] += rl[group, 0]
        acc[group, 3, half[1]] += rl[group, 1]
        for d, tile, side, part in ((1, 1, 0, 0), (-1, 3, 1, 1)):
            src, dst = acc.at[group, tile, half[part]], rs.at[group, side, half[part]]
            go(src, dst, rs_send, rs_recv.at[group], device(dy=d))

    def store(dx):
        group, xx = GROUP[dx], block(dx, 0)[0]
        arrive(rs.at[group], rs_recv.at[group])
        value = acc[group, 0] + rs[group, 0] + rs[group, 1]
        value = value * wa[0, xx].astype(jnp.float32)
        cols = pl.ds(pl.multiple_of(xx * 128, 128), 128)
        out_ref[:, cols] = value.astype(jnp.bfloat16)

    def bits_stage(stage):
        if stage == 0:
            for to in XY:
                ref = ixy.at[x * NY + y]
                go(ref, ref, info_send.at[0], info_recv.at[0], device(**to))
            return
        if stage == 1:
            arrive(ixy.at[pl.ds(0, len(XY))], info_recv.at[0])
            rows = pl.ds((z * 2 + c) * NX, NX)
            for k in range(NX):
                line = [ixy[k * NY + n] for n in range(NY)]
                info[(z * 2 + c) * NX + k] = line[0] + line[1] + line[2] + line[3]
            for to in ZC:
                go(info.at[rows], info.at[rows], info_send.at[1], info_recv.at[1], device(**to))
            return
        arrive(info.at[pl.ds(0, NX * len(ZC))], info_recv.at[1])
        line = lax.broadcasted_iota(jnp.int32, (64, 128), 0)
        lanes = lax.broadcasted_iota(jnp.int32, (64, 128), 1)
        table = jnp.zeros((64, 128), jnp.float32)
        for i in range(64):
            xi, zi, ci = i // 16, (i // 2) % 8, i % 2
            table = jnp.where(line == i, info[(zi * 2 + ci) * NX + xi], table)
        tail = lanes >= 64
        bp = jnp.where(tail & (table > 1.5), 1.0, 0.0)
        wp = jnp.where(tail, table - 2.0 * bp, 0.0)
        ap = jnp.where(tail, 0.0, table).astype(jnp.bfloat16)
        wide = jnp.concatenate([bp, jnp.zeros_like(bp)], axis=0).astype(jnp.bfloat16)
        link = jnp.dot(ap, wide, preferred_element_type=jnp.float32)
        present = jnp.where(link > 0.5, wp, 0.0)
        left = (
            lax.broadcasted_iota(jnp.int32, (128, 128), 0)
            < lax.broadcasted_iota(jnp.int32, (128, 128), 1)
        )
        marks = present.astype(jnp.bfloat16)
        inside = jnp.dot(marks, jnp.where(left, 1.0, 0.0).astype(jnp.bfloat16),
                         preferred_element_type=jnp.float32)
        own = line == row
        earlier = jnp.sum(jnp.where(line < row, present, 0.0))
        before = jnp.sum(jnp.where(own, inside, 0.0), axis=0, keepdims=True) + earlier
        here = jnp.sum(jnp.where(own, present, 0.0), axis=0, keepdims=True)
        slots = jnp.where(here > 0.5, before, -1.0)
        for t in range(2):
            here = jnp.where(lane == 64 + 2 * y + t, slots, 0.0)
            slot_ref[:, pl.ds(t, 1)] = jnp.sum(here, axis=1, keepdims=True)

    def sum_stage(k):
        if k == 0:
            value = jnp.sum(tot[...], axis=0, keepdims=True)
            first, size, mine, peers = 0, 16, z * 2 + c, ZC
        else:
            arrive(ta.at[pl.ds(16 * (k - 1), 15)], sum_recv.at[k - 1])
            value = ta[16 * (k - 1)]
            for n in range(1, 16):
                value = value + ta[16 * (k - 1) + n]
            first, size, mine, peers = 16, 16, x * NY + y, XY
        if k == 2:
            total_ref[0, 0] = jnp.sum(value) / (TILE * math.sqrt(64 * 8))
            return
        ta[first + mine] = value
        for to in peers:
            ref = ta.at[first + mine]
            go(ref, ref, sum_send, sum_recv.at[k], device(**to))

    run = {
        "step": step, "prepare": prepare, "multiply": multiply,
        "weights": weights, "scatter": scatter, "add": add, "store": store,
        "bits": bits_stage, "sum": sum_stage,
    }
    for kind, what in program():
        run[kind](what)
    gone(bg.at[pl.ds(0, (2 * MOVED + 1) * 1024)], bulk_send)
    gone(acc.at[pl.ds(0, 3)], rs_send)
    gone(wa.at[pl.ds(0, 3)], w_send)
    gone(ixy.at[pl.ds(0, 15)], info_send.at[0])
    gone(info.at[pl.ds(0, 60)], info_send.at[1])
    gone(ta.at[pl.ds(0, 30)], sum_send)
    for d in (1, 2, 3):
        move(d).wait_send()

    @pl.when(jnp.logical_not(diagonal))
    def _():
        move(0).wait_send()


def hand_over(masked, slot, masked_out, slot_out, sem):
    copies = [
        pltpu.make_async_copy(src, dst, sem.at[n])
        for n, (src, dst) in enumerate(((masked, masked_out), (slot, slot_out)))
    ]
    for copy in copies:
        copy.start()
    for copy in copies:
        copy.wait()


def on_device(a_values, a_present, b_values, b_present, w_values, w_present):
    hbm = pl.BlockSpec(memory_space=pltpu.HBM)
    smem = pl.BlockSpec(memory_space=pltpu.SMEM)
    vmem = pl.BlockSpec(memory_space=pltpu.VMEM)
    dma = pltpu.SemaphoreType.DMA
    bf16, f32, i32 = jnp.bfloat16, jnp.float32, jnp.int32
    masked, slot, total = pl.pallas_call(
        kernel,
        out_shape=(
            jax.ShapeDtypeStruct((TILE, 512), bf16),
            jax.ShapeDtypeStruct((1, 2), f32),
            jax.ShapeDtypeStruct((1, 1), f32),
        ),
        in_specs=[hbm] * 6,
        out_specs=(vmem, vmem, smem),
        scratch_shapes=[
            pltpu.VMEM((NX * NZ * 2 * 1024, 128), bf16),
            pltpu.VMEM((NZ, TILE, 2 * TILE), bf16),
            pltpu.VMEM((NX, NY, TILE, 128), f32),
            pltpu.VMEM((NX, 2, 128, 128), f32),
            pltpu.VMEM((NX, 2, TILE, 128), f32),
            pltpu.VMEM((NY, NX, TILE, 128), bf16),
            pltpu.VMEM((NX, TILE, 128), bf16),
            pltpu.VMEM((TILE, 512), bf16),
            pltpu.VMEM((TILE, 512), bf16),
            pltpu.VMEM((8, 128), f32),
            pltpu.VMEM((NX * NY, 1, 128), f32),
            pltpu.VMEM((64, 1, 128), f32),
            pltpu.VMEM((32, 1, 128), f32),
            pltpu.SMEM((1, 16), i32),
            pltpu.SMEM((1, 2), i32),
            pltpu.SMEM((1, 2), i32),
            dma, dma((5,)), dma((NX,)), dma((NY,)),
            dma, dma((len(KEY_ID),)), dma((len(BLOCKS),)),
            dma, dma, dma, dma((NX,)), dma((NX,)),
            dma((2,)), dma((2,)), dma, dma((2,)),
        ],
        compiler_params=pltpu.CompilerParams(
            collective_id=0, has_side_effects=True, vmem_limit_bytes=48 * 2**20
        ),
    )(*[
        pltpu.with_memory_space_constraint(v, pltpu.HBM)
        for v in (a_values, a_present, b_values, b_present, w_values, w_present)
    ])
    masked, slot = pl.pallas_call(
        hand_over,
        out_shape=(
            jax.ShapeDtypeStruct((TILE, 512), bf16),
            jax.ShapeDtypeStruct((1, 2), f32),
        ),
        in_specs=[vmem] * 2,
        out_specs=(hbm, hbm),
        scratch_shapes=[dma((2,))],
        compiler_params=pltpu.CompilerParams(vmem_limit_bytes=2**20),
    )(masked, slot)
    return masked, slot, total.reshape(())


def solution(mesh):
    spec = P("row", "col")
    return jax.shard_map(
        on_device, mesh=mesh, in_specs=(spec,) * 6, out_specs=(spec, spec, P()),
        check_vma=False,
    )
```
